128 devices in a mesh: dp: 8 (over x, z_lo), rep: 16 (over z_hi, y, core).
Axes of the slice: x: 4, y: 4, z: 4 (z_hi: 2, z_lo: 2; z = z_hi * 2 + z_lo), core: 2. Of those that a mesh axis runs over, the one named last changes fastest.
Arguments:
- queries: bfloat16 [65536, 2048], P(('dp', 'rep')), may hold values from -32 to 32
- key_rows: bfloat16 [65536, 2048], P(('dp', 'rep')), may hold values from -32 to 32
- values: bfloat16 [65536, 2048], P(('dp', 'rep')), may hold values from -6 to 6
- upstream: bfloat16 [65536, 2048], P(('dp', 'rep')), may hold values from -24 to 24
- out_weight: bfloat16 [2048, 2048], P(('dp', 'rep')), may hold values from -0.125 to 0.125
- sample_ids: int32 [128, 512], P(('dp', 'rep')), may hold values from 0 to 3, as said below
Outputs:
- grad_queries: bfloat16 [65536, 2048], P(('dp', 'rep'))
- grad_keys: bfloat16 [65536, 2048], P(('dp', 'rep'))
- grad_values: bfloat16 [65536, 2048], P(('dp', 'rep'))
- grad_weight: float32 [2048, 2048], P(('dp', 'rep'))
The draws below stay inside these ranges and needn't reach their ends.
Inputs may be any that keep to these rules, and one draw needn't show every extreme that they name: `sample_ids`: within a row the ids never fall, every row starts with 0 and ends with 3, and the tokens of one sample are contiguous.
All inputs are finite; a program needn't handle non-finite values.
Results may differ from the reference program's by a relative error of at most 0.015.
Values may be sent and summed in bfloat16 or wider, within the bound.
No kernel may reach another device: no remote copies, remote signals or barrier semaphores. Data moves between devices by JAX's collectives and lax.ppermute only.
A program may use at most 192 MiB of HBM per device.

```python
import math
import jax
import jax.numpy as jnp
from jax import lax

D = 2048
H = 16
DH = 128
HD = 2048
LEN = 512
NSEG = 4
SEQS = 128
TOKENS = 65536


def draw_queries(key, part):
    normal_part = jnp.clip(jax.random.normal(jax.random.fold_in(key, 11), (SEQS, LEN, H, DH), jnp.float32), -4.0, 4.0)
    normal_part = jnp.clip(normal_part, -32.0, 32.0)
    return normal_part.reshape(SEQS * LEN, H * DH).astype(jnp.bfloat16)


def draw_key_rows(key, part):
    normal_part = jnp.clip(jax.random.normal(jax.random.fold_in(key, 17), (SEQS, LEN, H, DH), jnp.float32), -4.0, 4.0)
    normal_part = jnp.clip(normal_part, -32.0, 32.0)
    return normal_part.reshape(SEQS * LEN, H * DH).astype(jnp.bfloat16)


def draw_sample_ids(key, part):
    cut_points = jax.random.randint(jax.random.fold_in(key, 29), (SEQS, NSEG - 1), LEN // 8, LEN - LEN // 8)
    positions = jnp.arange(LEN, dtype=jnp.int32)
    passed = (positions[None, :, None] >= cut_points[:, None, :]).astype(jnp.int32)
    return jnp.sum(passed, axis=2).astype(jnp.int32)


def with_spikes(array, own_key, source, target, parts, factor):
    def block_of(axis_at):
        return (jnp.arange(array.shape[axis_at]) // (array.shape[axis_at] // parts)).reshape((-1,) + (1,) * (array.ndim - 1 - axis_at))

    first = jax.random.permutation(own_key, parts)[block_of(target)]
    second = (block_of(target) + parts // 2) % parts
    return jnp.where((block_of(source) == first) | (block_of(source) == second), factor * array, array)


def shard_levels(rng, extent, shards, smallest, largest):
    level = 1.0
    for axis_at, parts in shards:
        draws = jax.random.uniform(jax.random.fold_in(jax.random.fold_in(rng, 6), axis_at), (parts,), jnp.float32, smallest / len(shards), largest / len(shards))
        level = level * jnp.repeat(jnp.exp(draws), extent[axis_at] // parts).reshape((-1,) + (1,) * (len(extent) - 1 - axis_at))
    return level


def bell_draw(stream_key, shape, scale, most, cuts=(), kind=jnp.bfloat16):
    result = scale * jax.random.normal(stream_key, shape, jnp.float32)
    if cuts:
        result = result * shard_levels(stream_key, shape, cuts, -0.22, 0.18)
    return jnp.clip(result, -most, most).astype(kind)


def gaussian_with(stream_key, extent, deviation, limit, pieces, heavy, kind=jnp.bfloat16):
    values = deviation * jax.random.normal(stream_key, extent, jnp.float32)
    if pieces:
        values = values * shard_levels(stream_key, extent, pieces, -0.22, 0.18)
    return jnp.clip(with_spikes(values, jax.random.fold_in(stream_key, 3), *heavy), -limit, limit).astype(kind)


def setup_inputs(seed: int = 0) -> dict:
    streams_of = jax.random.split(jax.random.key(seed), 7)
    return {
        "queries": draw_queries(jax.random.fold_in(streams_of[6], 71), 0),
        "key_rows": draw_key_rows(jax.random.fold_in(streams_of[6], 71), 0),
        "values": bell_draw(streams_of[2], (TOKENS, HD), 1.0, 6.0, ((0, 128),)),
        "upstream": gaussian_with(streams_of[3], (TOKENS, D), 1.0, 24.0, ((0, 128),), (0, 1, 128, 5.5)),
        "out_weight": bell_draw(streams_of[4], (D, HD), HD ** -0.5, 0.125, ((0, 128),)),
        "sample_ids": draw_sample_ids(jax.random.fold_in(streams_of[6], 71), 0),
    }


def sequence_pass(seq_block):
    query_block, key_block, value_block, grad_block, ids_row = seq_block
    scaling = 1.0 / math.sqrt(DH)
    query_wide = query_block.astype(jnp.float32)
    key_wide = key_block.astype(jnp.float32)
    value_wide = value_block.astype(jnp.float32)
    grad_wide = grad_block.astype(jnp.float32)
    positions = jnp.arange(LEN, dtype=jnp.int32)
    causal = positions[None, :] <= positions[:, None]
    allowed = jnp.logical_and(causal, ids_row[None, :] == ids_row[:, None])[None]
    scores = jnp.einsum('qhd,khd->hqk', query_wide, key_wide) * scaling
    masked = jnp.where(allowed, scores, -jnp.inf)
    row_max = lax.optimization_barrier(jnp.max(masked, axis=2, keepdims=True))
    raised = jnp.where(allowed, jnp.exp(masked - row_max), 0.0)
    probabilities = raised / lax.optimization_barrier(jnp.sum(raised, axis=2, keepdims=True))
    probs_low = lax.optimization_barrier(probabilities.astype(jnp.bfloat16)).astype(jnp.float32)
    attended = jnp.einsum('hqk,khd->qhd', probs_low, value_wide).astype(jnp.bfloat16)
    grad_values = jnp.einsum('hqk,qhd->khd', probs_low, grad_wide).astype(jnp.bfloat16)
    grad_probs = jnp.einsum('qhd,khd->hqk', grad_wide, value_wide)
    row_inner = lax.optimization_barrier(jnp.sum(probabilities * grad_probs, axis=2, keepdims=True))
    grad_scores = lax.optimization_barrier((probabilities * (grad_probs - row_inner)).astype(jnp.bfloat16)).astype(jnp.float32)
    grad_queries = (scaling * jnp.einsum('hqk,khd->qhd', grad_scores, key_wide)).astype(jnp.bfloat16)
    grad_keys = (scaling * jnp.einsum('hqk,qhd->khd', grad_scores, query_wide)).astype(jnp.bfloat16)
    return (attended, grad_queries, grad_keys, grad_values)

def reference(queries, key_rows, values, upstream, out_weight, sample_ids):
    grad_attended = jnp.dot(upstream, out_weight, preferred_element_type=jnp.float32).astype(jnp.bfloat16)
    grad_attended = lax.optimization_barrier(grad_attended)
    split_shape = (SEQS, LEN, H, DH)
    results = lax.map(sequence_pass, (queries.reshape(split_shape), key_rows.reshape(split_shape), values.reshape(split_shape), grad_attended.reshape(split_shape), sample_ids))
    attended, grad_queries, grad_keys, grad_values = [stacked.reshape(TOKENS, H * DH) for stacked in results]
    grad_weight = jnp.dot(upstream.T, attended, preferred_element_type=jnp.float32) / math.sqrt(TOKENS)
    return (grad_queries, grad_keys, grad_values, grad_weight)
```

```python
import functools
import math

import jax
import jax.numpy as jnp
from jax import lax
from jax.experimental import pallas as pl
from jax.experimental.pallas import tpu as pltpu
from jax.sharding import Mesh
from jax.sharding import PartitionSpec as P


H = 16
DH = 128
HALF = 8
SCALE = 1.0 / math.sqrt(DH)
LOG2E = math.log2(math.e)
BF = jnp.bfloat16
F32 = jnp.float32
BLOCKS = ((0, 11), (11, 22), (22, 32))
DELTAS = (1, 3, 2)


def coords(i):
    return (i // 32, (i // 2) % 4, 2 * ((i // 8) % 2) + (i // 16) % 2, i % 2)


def device_at(x, y, z, core):
    x, y, z = x % 4, y % 4, z % 4
    return x * 32 + (z % 2) * 16 + (z // 2) * 8 + y * 2 + core


COSETS = [
    [device_at(s // 4, s % 4, q - s // 4 - s % 4, core) for s in range(16) for core in range(2)]
    for q in range(4)
]
CORE_SWAP = [(i, i ^ 1) for i in range(128)]


def shift(axis, by):
    pairs = []
    for i in range(128):
        place = list(coords(i))
        place[axis] += by
        pairs.append((i, device_at(*place)))
    return pairs


def exchange(pieces):
    return lax.all_to_all(pieces, "d", 0, 0, axis_index_groups=COSETS, tiled=True)


def params(vmem_mib=56):
    return pltpu.CompilerParams(
        dimension_semantics=("arbitrary",), vmem_limit_bytes=vmem_mib * 1024 * 1024
    )


def forward_kernel(base, q_ref, k_ref, v_ref, first_ref, att_ref, prob_ref, bias_ref):
    rows = q_ref.shape[0]

    @pl.when(pl.program_id(0) == 0)
    def _():
        t = lax.broadcasted_iota(jnp.int32, (rows, rows), 0)
        u = lax.broadcasted_iota(jnp.int32, (rows, rows), 1)
        allowed = jnp.logical_and(u <= t, u >= first_ref[...])
        bias_ref[...] = jnp.where(allowed, 0.0, -1e30)

    block = 256
    for i in range(rows // block):
        lo, hi = i * block, (i + 1) * block
        scores = lax.dot_general(
            q_ref[lo:hi, :], k_ref[:hi, :], (((1,), (1,)), ((), ())), preferred_element_type=F32
        )
        scores = scores * (SCALE * LOG2E) + bias_ref[lo:hi, :hi]
        top = jnp.max(scores, axis=1, keepdims=True)
        raised = jnp.exp2(scores - top)
        total = jnp.sum(raised, axis=1, keepdims=True)
        probs = (raised * (1.0 / total)).astype(BF)
        prob_ref[0, lo:hi, :hi] = probs
        att_ref[lo:hi, :] = jnp.dot(
            probs, v_ref[:hi, :], preferred_element_type=F32
        ).astype(BF)


def attend_forward(base, queries, keys, values, first):
    rows = queries.shape[0]
    head = pl.BlockSpec((rows, DH), lambda i, b: (0, b[0] + i))
    return pl.pallas_call(
        forward_kernel,
        grid_spec=pltpu.PrefetchScalarGridSpec(
            num_scalar_prefetch=1,
            grid=(HALF,),
            in_specs=[head, head, head, pl.BlockSpec((rows, 1), lambda i, b: (0, 0))],
            out_specs=[
                pl.BlockSpec((rows, DH), lambda i, b: (0, i)),
                pl.BlockSpec((1, rows, rows), lambda i, b: (i, 0, 0)),
            ],
            scratch_shapes=[pltpu.VMEM((rows, rows), F32)],
        ),
        out_shape=[
            jax.ShapeDtypeStruct((rows, HALF * DH), BF),
            jax.ShapeDtypeStruct((HALF, rows, rows), BF),
        ],
        compiler_params=params(),
        cost_estimate=pl.CostEstimate(
            flops=2 * 2 * HALF * rows * rows * DH, bytes_accessed=9 << 20, transcendentals=1 << 20
        ),
        name="attend_forward",
    )(base, queries, keys, values, first)


def backward_kernel(base, q_ref, k_ref, v_ref, g_ref, att_ref, prob_ref, *refs):
    dq_ref, dk_ref, dv_ref = refs[-3:]
    rows = q_ref.shape[0]
    grad = g_ref[...]
    inner = jnp.sum(grad.astype(F32) * att_ref[...].astype(F32), axis=1, keepdims=True)
    grad_t = grad.T
    query_t = q_ref[...].T
    block = 256
    dv_t = []
    dk_t = []
    for i in range(rows // block):
        lo, hi = i * block, (i + 1) * block
        probs = prob_ref[0, lo:hi, :hi]
        grad_probs = lax.dot_general(
            grad[lo:hi, :], v_ref[:hi, :], (((1,), (1,)), ((), ())), preferred_element_type=F32
        )
        grad_scores = (probs.astype(F32) * (grad_probs - inner[lo:hi, :])).astype(BF)
        dq_ref[lo:hi, :] = (
            SCALE * jnp.dot(grad_scores, k_ref[:hi, :], preferred_element_type=F32)
        ).astype(BF)
        dv_t.append(jnp.dot(grad_t[:, lo:hi], probs, preferred_element_type=F32))
        dk_t.append(jnp.dot(query_t[:, lo:hi], grad_scores, preferred_element_type=F32))
    for out_ref, parts, factor in ((dv_ref, dv_t, 1.0), (dk_ref, dk_t, SCALE)):
        for j in range(rows // block):
            lo, hi = j * block, (j + 1) * block
            total = parts[j][:, lo:hi]
            for part in parts[j + 1 :]:
                total = total + part[:, lo:hi]
            out_ref[lo:hi, :] = (total * factor).astype(BF).T


def attend_backward(base, queries, keys, values, grad, attended, probs, previous):
    rows = queries.shape[0]
    head = pl.BlockSpec((rows, DH), lambda i, b: (0, b[0] + i))
    half = pl.BlockSpec((rows, DH), lambda i, b: (0, i))
    shape = jax.ShapeDtypeStruct(queries.shape, BF)
    return pl.pallas_call(
        backward_kernel,
        grid_spec=pltpu.PrefetchScalarGridSpec(
            num_scalar_prefetch=1,
            grid=(HALF,),
            in_specs=[head, head, head, half, half]
            + [pl.BlockSpec((1, rows, rows), lambda i, b: (i, 0, 0))]
            + [pl.BlockSpec(memory_space=pl.ANY)] * len(previous),
            out_specs=[head, head, head],
        ),
        out_shape=[shape, shape, shape],
        input_output_aliases={7 + n: n for n in range(len(previous))},
        compiler_params=params(),
        cost_estimate=pl.CostEstimate(
            flops=4 * 2 * HALF * rows * rows * DH, bytes_accessed=12 << 20, transcendentals=0
        ),
        name="attend_backward",
    )(base, queries, keys, values, grad, attended, probs, *previous)


def row_of(place, delta, block):
    s, core = block // 2, block % 2
    x, y = s // 4, s % 4
    z = (place + (delta - x - y) % 4) % 4
    return 16 * (x * 32 + (z % 2) * 16 + (z // 2) * 8 + y * 2 + core)


def parts_of_cosets():
    yield 0, 0, 32
    for delta in DELTAS:
        for lo, hi in BLOCKS:
            yield delta, lo, hi


def project_kernel(coset, up_own_ref, up_other_ref, *refs):
    pieces, (own_ref, other_ref, weight_ref) = refs[:10], refs[10:]
    for ref, (delta, lo, hi) in zip(pieces, parts_of_cosets()):
        for block in range(lo, hi):
            row = pl.multiple_of(row_of(coset[0], delta, block), 16)
            weight_ref[pl.ds(row, 16), :] = ref[16 * (block - lo) : 16 * (block - lo + 1), :]
    weight = weight_ref[...]
    other_ref[...] = jnp.dot(up_other_ref[...], weight, preferred_element_type=F32).astype(BF)
    own_ref[...] = jnp.dot(up_own_ref[...], weight, preferred_element_type=F32).astype(BF)


def project(coset, up_own, up_other, pieces):
    rows, width = up_own.shape
    cols = pieces[0].shape[1]
    step = 256
    whole = pl.BlockSpec((rows, width), lambda i, b: (0, 0))
    out = pl.BlockSpec((rows, step), lambda i, b: (0, i))
    return pl.pallas_call(
        project_kernel,
        grid_spec=pltpu.PrefetchScalarGridSpec(
            num_scalar_prefetch=1,
            grid=(cols // step,),
            in_specs=[whole, whole]
            + [pl.BlockSpec((piece.shape[0], step), lambda i, b: (0, i)) for piece in pieces],
            out_specs=[out, out],
            scratch_shapes=[pltpu.VMEM((width, step), BF)],
        ),
        out_shape=[jax.ShapeDtypeStruct((rows, cols), BF)] * 2,
        compiler_params=params(),
        cost_estimate=pl.CostEstimate(
            flops=2 * 2 * rows * width * cols, bytes_accessed=10 << 20, transcendentals=0
        ),
        name="project",
    )(coset, up_own, up_other, *pieces)


def weight_kernel(coset, up_own_ref, up_other_ref, att_own_ref, att_other_ref, *refs):
    outs, (up_t_ref, sums_ref) = refs[:10], refs[10:]
    rows = up_own_ref.shape[0]

    @pl.when(pl.program_id(0) == 0)
    def _():
        up_t_ref[:, :rows] = up_own_ref[...].T
        up_t_ref[:, rows:] = up_other_ref[...].T

    attended = jnp.concatenate([att_own_ref[...], att_other_ref[...]], axis=0)
    sums_ref[...] = jnp.dot(up_t_ref[...], attended, preferred_element_type=F32).astype(BF)
    for ref, (delta, lo, hi) in zip(outs, parts_of_cosets()):
        for block in range(lo, hi):
            row = pl.multiple_of(row_of(coset[0], delta, block), 16)
            ref[16 * (block - lo) : 16 * (block - lo + 1), :] = sums_ref[pl.ds(row, 16), :]


def weight_sums(coset, up_own, up_other, att_own, att_other):
    rows, width = up_own.shape
    cols = att_own.shape[1]
    step = 256
    whole = pl.BlockSpec((rows, width), lambda i, b: (0, 0))
    att = pl.BlockSpec((rows, step), lambda i, b: (0, i))
    sizes = [16 * (hi - lo) for _, lo, hi in parts_of_cosets()]
    return pl.pallas_call(
        weight_kernel,
        grid_spec=pltpu.PrefetchScalarGridSpec(
            num_scalar_prefetch=1,
            grid=(cols // step,),
            in_specs=[whole, whole, att, att],
            out_specs=[pl.BlockSpec((size, step), lambda i, b: (0, i)) for size in sizes],
            scratch_shapes=[pltpu.VMEM((width, 2 * rows), BF), pltpu.VMEM((width, step), BF)],
        ),
        out_shape=[jax.ShapeDtypeStruct((size, cols), BF) for size in sizes],
        compiler_params=params(),
        cost_estimate=pl.CostEstimate(
            flops=2 * 2 * rows * width * cols, bytes_accessed=10 << 20, transcendentals=0
        ),
        name="weight_sums",
    )(coset, up_own, up_other, att_own, att_other)


def gather_weight(weight):
    cols = weight.shape[1] // 2
    halves = jnp.stack([weight[:, :cols], weight[:, cols:]])
    pieces = jnp.broadcast_to(halves[None], (16, 2, 16, cols)).reshape(32, 16, cols)
    block = exchange(pieces).reshape(512, cols)
    parts = [block[16 * lo : 16 * hi] for lo, hi in BLOCKS]
    result = [block]
    for delta in DELTAS:
        for axis in range(3):
            result.append(lax.ppermute(parts[axis], "d", shift(axis, -delta)))
    return result


def reduce_rows(pieces, total_tokens):
    cols = pieces[0].shape[1]
    received = [
        lax.ppermute(piece, "d", shift(n % 3, DELTAS[n // 3])) for n, piece in enumerate(pieces[1:])
    ]
    parts = []
    for axis, (lo, hi) in enumerate(BLOCKS):
        part = pieces[0][16 * lo : 16 * hi].astype(F32)
        for n in range(3):
            part = part + received[3 * n + axis].astype(F32)
        parts.append(part.astype(BF))
    block = jnp.concatenate(parts, axis=0).reshape(32, 16, cols)
    rows = exchange(block).reshape(16, 2, 16, cols).astype(F32)
    sums = jnp.sum(rows, axis=0) * (1.0 / math.sqrt(total_tokens))
    return jnp.concatenate([sums[0], sums[1]], axis=1)


def shards(queries, keys, values, upstream, weight, sample_ids):
    rows = queries.shape[0]
    me = lax.axis_index("d")
    core = me % 2
    z = 2 * ((me // 8) % 2) + (me // 16) % 2
    coset = ((me // 32 + (me // 2) % 4 + z) % 4).astype(jnp.int32).reshape(1)
    base_own = (HALF * core).astype(jnp.int32).reshape(1)
    base_other = (HALF * (1 - core)).astype(jnp.int32).reshape(1)
    ids = sample_ids[0]
    first = jnp.sum((ids[None, :] < ids[:, None]).astype(jnp.int32), axis=1, keepdims=True)

    up_other = lax.ppermute(upstream, "d", CORE_SWAP)
    gathered = gather_weight(weight)
    att_a, prob_a = attend_forward(base_other, queries, keys, values, first)
    att_other = lax.ppermute(att_a, "d", CORE_SWAP)
    att_b, prob_b = attend_forward(base_own, queries, keys, values, first)
    sums = weight_sums(coset, upstream, up_other, att_b, att_other)
    grad_own, grad_sent = project(coset, upstream, up_other, gathered)
    grad_other = lax.ppermute(grad_sent, "d", CORE_SWAP)
    grad_weight = reduce_rows(sums, rows * lax.axis_size("d"))
    outs = attend_backward(base_own, queries, keys, values, grad_own, att_b, prob_b, ())
    outs = attend_backward(base_other, queries, keys, values, grad_other, att_a, prob_a, tuple(outs))
    return (*outs, grad_weight)


def solution(mesh):
    flat = Mesh(mesh.devices.reshape(-1), ("d",))
    return jax.shard_map(
        shards,
        mesh=flat,
        in_specs=(P("d", None),) * 6,
        out_specs=(P("d", None),) * 4,
        check_vma=False,
    )
```

```python
import math

import jax
import jax.numpy as jnp
from jax import lax
from jax.experimental import pallas as pl
from jax.experimental.pallas import tpu as pltpu
from jax.sharding import Mesh
from jax.sharding import PartitionSpec as P


H = 16
DH = 128
HALF = 8
STEP_HEADS = 4
FLOPS_4US = 2 << 30
FLOPS_6US = 3 << 30
SCALE = 1.0 / math.sqrt(DH)
LOG2E = math.log2(math.e)
BF = jnp.bfloat16
F32 = jnp.float32
CLASSES = ((1, 0), (0, 1), (1, 1))


def coords(i):
    return (i // 32, (i // 2) % 4, 2 * ((i // 8) % 2) + (i // 16) % 2, i % 2)


def device_at(x, y, z, core):
    x, y, z = x % 4, y % 4, z % 4
    return x * 32 + (z % 2) * 16 + (z // 2) * 8 + y * 2 + core


COSETS = [
    [
        device_at((kx + z) % 2 + 2 * i, (ky + z) % 2 + 2 * j, z, core)
        for z in range(4)
        for i in range(2)
        for j in range(2)
        for core in range(2)
    ]
    for kx in range(2)
    for ky in range(2)
]
CORE_SWAP = [(i, i ^ 1) for i in range(128)]


def shift(axis, by):
    pairs = []
    for i in range(128):
        place = list(coords(i))
        place[axis] += by
        pairs.append((i, device_at(*place)))
    return pairs


def exchange(pieces):
    return lax.all_to_all(pieces, "d", 0, 0, axis_index_groups=COSETS, tiled=True)


def grid_params():
    return pltpu.CompilerParams(
        dimension_semantics=("arbitrary",), vmem_limit_bytes=28 * 1024 * 1024
    )


def whole_params(mib):
    return pltpu.CompilerParams(vmem_limit_bytes=mib * 1024 * 1024)


def forward_kernel(base, q_ref, k_ref, v_ref, ids_ref, att_ref, prob_ref, bias_ref):
    rows = q_ref.shape[0]

    @pl.when(pl.program_id(0) == 0)
    def _():
        t = lax.broadcasted_iota(jnp.int32, (rows, rows), 0)
        u = lax.broadcasted_iota(jnp.int32, (rows, rows), 1)
        ids = ids_ref[...].astype(F32)
        own = jnp.broadcast_to(ids, (DH, rows)).T[:, :1]
        bias_ref[...] = jnp.where(jnp.logical_and(u <= t, own == ids), 0.0, -1e30)

    block = 256

    def cut(h, i):
        return slice(h * DH, (h + 1) * DH), i * block, (i + 1) * block

    def scores_of(h, i):
        cols, lo, hi = cut(h, i)
        return lax.dot_general(
            q_ref[lo:hi, cols],
            k_ref[:hi, cols],
            (((1,), (1,)), ((), ())),
            preferred_element_type=F32,
        )

    def softmax_of(h, i, scores):
        _, lo, hi = cut(h, i)
        scores = scores * (SCALE * LOG2E) + bias_ref[lo:hi, :hi]
        raised = jnp.exp2(scores - jnp.max(scores, axis=1, keepdims=True))
        total = jnp.sum(raised, axis=1, keepdims=True)
        probs = (raised * (1.0 / total)).astype(BF)
        prob_ref[h, lo:hi, :hi] = probs
        return probs

    def attend(h, i, probs):
        cols, lo, hi = cut(h, i)
        att_ref[lo:hi, cols] = jnp.dot(
            probs, v_ref[:hi, cols], preferred_element_type=F32
        ).astype(BF)

    jobs = [(h, i) for h in range(STEP_HEADS) for i in range(rows // block)]
    ready = scores_of(*jobs[0])
    waiting = None
    for n, job in enumerate(jobs):
        scores = ready
        if n + 1 < len(jobs):
            ready = scores_of(*jobs[n + 1])
        probs = softmax_of(*job, scores)
        if waiting is not None:
            attend(*waiting)
        waiting = (*job, probs)
    attend(*waiting)


def attend_forward(base, queries, keys, values, ids):
    rows = queries.shape[0]
    head = pl.BlockSpec((rows, DH * STEP_HEADS), lambda i, b: (0, b[0] + i))
    return pl.pallas_call(
        forward_kernel,
        grid_spec=pltpu.PrefetchScalarGridSpec(
            num_scalar_prefetch=1,
            grid=(HALF // STEP_HEADS,),
            in_specs=[head, head, head, pl.BlockSpec((1, rows), lambda i, b: (0, 0))],
            out_specs=[
                pl.BlockSpec((rows, DH * STEP_HEADS), lambda i, b: (0, i)),
                pl.BlockSpec((STEP_HEADS, rows, rows), lambda i, b: (i, 0, 0)),
            ],
            scratch_shapes=[pltpu.VMEM((rows, rows), F32)],
        ),
        out_shape=[
            jax.ShapeDtypeStruct((rows, HALF * DH), BF),
            jax.ShapeDtypeStruct((HALF, rows, rows), BF),
        ],
        compiler_params=grid_params(),
        cost_estimate=pl.CostEstimate(
            flops=FLOPS_6US, bytes_accessed=9 << 20, transcendentals=1 << 20
        ),
        name="attend_forward",
    )(base, queries, keys, values, ids)


def backward_kernel(base, q_ref, k_ref, v_ref, g_ref, att_ref, prob_ref, *refs):
    dq_ref, dk_ref, dv_ref = refs[-3:]
    rows = q_ref.shape[0]
    block = 256
    count = rows // block
    inner, grad_t, query_t, sums = {}, {}, {}, {}

    def cut(h, i):
        return slice(h * DH, (h + 1) * DH), i * block, (i + 1) * block

    def prepare(h):
        cols = cut(h, 0)[0]
        grad = g_ref[:, cols]
        inner[h] = jnp.sum(
            grad.astype(F32) * att_ref[:, cols].astype(F32), axis=1, keepdims=True
        )
        grad_t[h] = grad.T
        query_t[h] = q_ref[:, cols].T
        sums[h] = []

    def grad_probs_of(h, i):
        cols, lo, hi = cut(h, i)
        return lax.dot_general(
            g_ref[lo:hi, cols],
            v_ref[:hi, cols],
            (((1,), (1,)), ((), ())),
            preferred_element_type=F32,
        )

    def grad_scores_of(h, i, grad_probs):
        _, lo, hi = cut(h, i)
        probs = prob_ref[h, lo:hi, :hi].astype(F32)
        return (probs * (grad_probs - inner[h][lo:hi, :])).astype(BF)

    def finish(h, i, grad_scores):
        cols, lo, hi = cut(h, i)
        probs = prob_ref[h, lo:hi, :hi]
        dq_ref[lo:hi, cols] = (
            SCALE * jnp.dot(grad_scores, k_ref[:hi, cols], preferred_element_type=F32)
        ).astype(BF)
        sums[h].append(
            (
                jnp.dot(grad_t[h][:, lo:hi], probs, preferred_element_type=F32),
                jnp.dot(query_t[h][:, lo:hi], grad_scores, preferred_element_type=F32),
            )
        )
        if i < count - 1:
            return
        for n, (out_ref, factor) in enumerate(((dv_ref, 1.0), (dk_ref, SCALE))):
            for j in range(count):
                _, lo, hi = cut(h, j)
                total = sums[h][j][n][:, lo:hi]
                for m in range(j + 1, count):
                    total = total + sums[h][m][n][:, lo:hi]
                out_ref[lo:hi, cols] = (total * factor).astype(BF).T

    jobs = [(h, i) for h in range(STEP_HEADS) for i in range(count)]
    prepare(0)
    ready = grad_probs_of(*jobs[0])
    waiting = None
    for n, job in enumerate(jobs):
        grad_probs = ready
        if n + 1 < len(jobs):
            if jobs[n + 1][1] == 0:
                prepare(jobs[n + 1][0])
            ready = grad_probs_of(*jobs[n + 1])
        grad_scores = grad_scores_of(*job, grad_probs)
        if waiting is not None:
            finish(*waiting)
        waiting = (*job, grad_scores)
    finish(*waiting)


def attend_backward(base, queries, keys, values, grad, attended, probs, previous):
    rows = queries.shape[0]
    head = pl.BlockSpec((rows, DH * STEP_HEADS), lambda i, b: (0, b[0] + i))
    half = pl.BlockSpec((rows, DH * STEP_HEADS), lambda i, b: (0, i))
    shape = jax.ShapeDtypeStruct(queries.shape, BF)
    return pl.pallas_call(
        backward_kernel,
        grid_spec=pltpu.PrefetchScalarGridSpec(
            num_scalar_prefetch=1,
            grid=(HALF // STEP_HEADS,),
            in_specs=[head, head, head, half, half]
            + [pl.BlockSpec((STEP_HEADS, rows, rows), lambda i, b: (i, 0, 0))]
            + [pl.BlockSpec(memory_space=pl.ANY)] * len(previous),
            out_specs=[head, head, head],
        ),
        out_shape=[shape, shape, shape],
        input_output_aliases={7 + n: n for n in range(len(previous))},
        compiler_params=grid_params(),
        cost_estimate=pl.CostEstimate(
            flops=FLOPS_4US, bytes_accessed=12 << 20, transcendentals=0
        ),
        name="attend_backward",
    )(base, queries, keys, values, grad, attended, probs, *previous)


def row_of(coset, other, block):
    core, j, i, z = block % 2, (block // 2) % 2, (block // 4) % 2, block // 8
    odd_x, odd_y = (z + other[0]) % 2, (z + other[1]) % 2
    x = (1 - coset[0] if odd_x else coset[0]) + 2 * i
    y = (1 - coset[1] if odd_y else coset[1]) + 2 * j
    return 16 * (x * 32 + (z % 2) * 16 + (z // 2) * 8 + y * 2 + core)


def coset_parts():
    yield (0, 0), 0, 32
    for other in CLASSES:
        yield other, 0, 16
        yield other, 16, 32


def project_kernel(coset, up_own_ref, up_other_ref, *refs):
    pieces, (own_ref, other_ref, weight_ref) = refs[:7], refs[7:]
    place = (coset[0], coset[1])
    for ref, (other, lo, hi) in zip(pieces, coset_parts()):
        for block in range(lo, hi):
            row = pl.multiple_of(row_of(place, other, block), 16)
            weight_ref[pl.ds(row, 16), :] = ref[16 * (block - lo) : 16 * (block - lo + 1), :]
    step = 512
    for up_ref, out_ref in ((up_other_ref, other_ref), (up_own_ref, own_ref)):
        for lo in range(0, out_ref.shape[1], step):
            out_ref[:, lo : lo + step] = jnp.dot(
                up_ref[...], weight_ref[:, lo : lo + step], preferred_element_type=F32
            ).astype(BF)


SMEM = pl.BlockSpec(memory_space=pltpu.SMEM)
VMEM = pl.BlockSpec(memory_space=pltpu.VMEM)


def project(coset, up_own, up_other, pieces):
    rows, width = up_own.shape
    cols = pieces[0].shape[1]
    return pl.pallas_call(
        project_kernel,
        in_specs=[SMEM] + [VMEM] * (2 + len(pieces)),
        out_specs=[VMEM] * 2,
        out_shape=[jax.ShapeDtypeStruct((rows, cols), BF)] * 2,
        scratch_shapes=[pltpu.VMEM((width, cols), BF)],
        compiler_params=whole_params(12),
        cost_estimate=pl.CostEstimate(
            flops=FLOPS_4US, bytes_accessed=10 << 20, transcendentals=0
        ),
        name="project",
    )(coset, up_own, up_other, *pieces)


def weight_kernel(coset, up_own_ref, up_other_ref, att_own_ref, att_other_ref, *refs):
    outs, sums_ref = refs[:7], refs[7]
    width = up_own_ref.shape[1]
    place = (coset[0], coset[1])
    step, cut = 256, 512

    def strip(lo):
        return jnp.concatenate(
            [up_own_ref[:, lo : lo + step].T, up_other_ref[:, lo : lo + step].T], axis=1
        )

    ready = strip(0)
    for lo in range(0, width, step):
        up_t = ready
        if lo + step < width:
            ready = strip(lo + step)
        for col in range(0, sums_ref.shape[1], cut):
            attended = jnp.concatenate(
                [att_own_ref[:, col : col + cut], att_other_ref[:, col : col + cut]], axis=0
            )
            sums_ref[lo : lo + step, col : col + cut] = jnp.dot(
                up_t, attended, preferred_element_type=F32
            ).astype(BF)
    for ref, (other, lo, hi) in zip(outs, coset_parts()):
        for block in range(lo, hi):
            row = pl.multiple_of(row_of(place, other, block), 16)
            ref[16 * (block - lo) : 16 * (block - lo + 1), :] = sums_ref[pl.ds(row, 16), :]


def weight_sums(coset, up_own, up_other, att_own, att_other):
    width = up_own.shape[1]
    cols = att_own.shape[1]
    sizes = [16 * (hi - lo) for _, lo, hi in coset_parts()]
    return pl.pallas_call(
        weight_kernel,
        in_specs=[SMEM] + [VMEM] * 4,
        out_specs=[VMEM] * len(sizes),
        out_shape=[jax.ShapeDtypeStruct((size, cols), BF) for size in sizes],
        scratch_shapes=[pltpu.VMEM((width, cols), BF)],
        compiler_params=whole_params(12),
        cost_estimate=pl.CostEstimate(
            flops=FLOPS_4US, bytes_accessed=10 << 20, transcendentals=0
        ),
        name="weight_sums",
    )(coset, up_own, up_other, att_own, att_other)


def spread_kernel(weight_ref, out_ref):
    cols = out_ref.shape[2]
    for n in range(out_ref.shape[0]):
        out_ref[n] = weight_ref[:, cols * (n % 2) : cols * (n % 2 + 1)]


def gather_weight(weight):
    rows, cols = weight.shape[0], weight.shape[1] // 2
    pieces = pl.pallas_call(
        spread_kernel,
        in_specs=[VMEM],
        out_specs=VMEM,
        out_shape=jax.ShapeDtypeStruct((32, rows, cols), BF),
        compiler_params=whole_params(2),
        name="spread",
    )(weight)
    block = exchange(pieces).reshape(32 * rows, cols)
    parts = (block[: 16 * rows], block[16 * rows :])
    result = [block]
    for axis in range(3):
        result.append(lax.ppermute(parts[0], "d", shift(axis, -1)))
        result.append(lax.ppermute(parts[1], "d", shift(axis, 1)))
    return result


def add_kernel(own_ref, *refs):
    received, out_ref = refs[:6], refs[6]
    rows = received[0].shape[0]
    for half in range(2):
        for lo in range(0, rows, 16):
            total = own_ref[rows * half + lo : rows * half + lo + 16, :].astype(F32)
            for axis in range(3):
                total = total + received[2 * axis + half][lo : lo + 16, :].astype(F32)
            out_ref[rows * half + lo : rows * half + lo + 16, :] = total.astype(BF)


def reduce_rows(pieces, total_tokens):
    cols = pieces[0].shape[1]
    received = [
        lax.ppermute(piece, "d", shift(n // 2, 1 - 2 * (n % 2)))
        for n, piece in enumerate(pieces[1:])
    ]
    block = pl.pallas_call(
        add_kernel,
        in_specs=[VMEM] * 7,
        out_specs=VMEM,
        out_shape=jax.ShapeDtypeStruct(pieces[0].shape, BF),
        compiler_params=whole_params(2),
        name="add_received",
    )(pieces[0], *received)
    rows = exchange(block.reshape(32, -1, cols)).reshape(16, 2, -1, cols).astype(F32)
    sums = jnp.sum(rows, axis=0) * (1.0 / math.sqrt(total_tokens))
    return jnp.concatenate([sums[0], sums[1]], axis=1)


def shards(queries, keys, values, upstream, weight, sample_ids):
    rows = queries.shape[0]
    me = lax.axis_index("d")
    core = jnp.bitwise_and(me, 1)
    z = jnp.bitwise_and(jnp.right_shift(me, 4), 1)
    kx = jnp.bitwise_and(jnp.right_shift(me, 5) + z, 1)
    ky = jnp.bitwise_and(jnp.right_shift(me, 1) + z, 1)
    coset = jnp.stack([kx, ky]).astype(jnp.int32)
    steps = HALF // STEP_HEADS
    base_own = (steps * core).astype(jnp.int32).reshape(1)
    base_other = (steps * (1 - core)).astype(jnp.int32).reshape(1)

    up_other = lax.ppermute(upstream, "d", CORE_SWAP)
    gathered = gather_weight(weight)
    att_a, prob_a = attend_forward(base_other, queries, keys, values, sample_ids)
    att_other = lax.ppermute(att_a, "d", CORE_SWAP)
    att_b, prob_b = attend_forward(base_own, queries, keys, values, sample_ids)
    sums = weight_sums(coset, upstream, up_other, att_b, att_other)
    grad_own, grad_sent = project(coset, upstream, up_other, gathered)
    grad_other = lax.ppermute(grad_sent, "d", CORE_SWAP)
    grad_weight = reduce_rows(sums, rows * lax.axis_size("d"))
    outs = attend_backward(base_own, queries, keys, values, grad_own, att_b, prob_b, ())
    outs = attend_backward(base_other, queries, keys, values, grad_other, att_a, prob_a, tuple(outs))
    return (*outs, grad_weight)


def solution(mesh):
    flat = Mesh(mesh.devices.reshape(-1), ("d",))
    return jax.shard_map(
        shards,
        mesh=flat,
        in_specs=(P("d", None),) * 6,
        out_specs=(P("d", None),) * 4,
        check_vma=False,
    )
```

```python
import math

import jax
import jax.numpy as jnp
from jax import lax
from jax.experimental import pallas as pl
from jax.experimental.pallas import tpu as pltpu
from jax.sharding import Mesh
from jax.sharding import PartitionSpec as P


DH = 128
HALF = 8
STEP_HEADS = 4
LIMIT = 50
FLOPS_4US = 2 << 30
FLOPS_6US = 3 << 30
SCALE = 1.0 / math.sqrt(DH)
LOG2E = math.log2(math.e)
BF = jnp.bfloat16
F32 = jnp.float32
CLASSES = ((1, 0), (0, 1), (1, 1))


def coords(i):
    return (i // 32, (i // 2) % 4, 2 * ((i // 8) % 2) + (i // 16) % 2, i % 2)


def device_at(x, y, z, core):
    x, y, z = x % 4, y % 4, z % 4
    return x * 32 + (z % 2) * 16 + (z // 2) * 8 + y * 2 + core


COSETS = [
    [
        device_at((kx + z) % 2 + 2 * i, (ky + z) % 2 + 2 * j, z, core)
        for z in range(4)
        for i in range(2)
        for j in range(2)
        for core in range(2)
    ]
    for kx in range(2)
    for ky in range(2)
]
CORE_SWAP = [(i, i ^ 1) for i in range(128)]


def shift(axis, by):
    pairs = []
    for i in range(128):
        place = list(coords(i))
        place[axis] += by
        pairs.append((i, device_at(*place)))
    return pairs


def exchange(pieces):
    return lax.all_to_all(pieces, "d", 0, 0, axis_index_groups=COSETS, tiled=True)


def grid_params():
    return pltpu.CompilerParams(
        dimension_semantics=("arbitrary",), vmem_limit_bytes=LIMIT * 1024 * 1024
    )


def whole_params(mib):
    return pltpu.CompilerParams(vmem_limit_bytes=mib * 1024 * 1024)


def forward_kernel(base, q_ref, k_ref, v_ref, ids_ref, att_ref, prob_ref, bias_ref):
    rows = q_ref.shape[0]

    @pl.when(pl.program_id(0) == 0)
    def _():
        t = lax.broadcasted_iota(jnp.int32, (rows, rows), 0)
        u = lax.broadcasted_iota(jnp.int32, (rows, rows), 1)
        ids = ids_ref[...].astype(F32)
        own = jnp.broadcast_to(ids, (DH, rows)).T[:, :1]
        bias_ref[...] = jnp.where(jnp.logical_and(u <= t, own == ids), 0.0, -1e30)

    block = 256

    def cut(h, i):
        return slice(h * DH, (h + 1) * DH), i * block, (i + 1) * block

    def scores_of(h, i):
        cols, lo, hi = cut(h, i)
        return lax.dot_general(
            q_ref[lo:hi, cols],
            k_ref[:hi, cols],
            (((1,), (1,)), ((), ())),
            preferred_element_type=F32,
        )

    def softmax_of(h, i, scores):
        _, lo, hi = cut(h, i)
        scores = scores * (SCALE * LOG2E) + bias_ref[lo:hi, :hi]
        raised = jnp.exp2(scores - jnp.max(scores, axis=1, keepdims=True))
        total = jnp.sum(raised, axis=1, keepdims=True)
        probs = (raised * (1.0 / total)).astype(BF)
        prob_ref[h, lo:hi, :hi] = probs
        return probs

    def attend(h, i, probs):
        cols, lo, hi = cut(h, i)
        att_ref[lo:hi, cols] = jnp.dot(
            probs, v_ref[:hi, cols], preferred_element_type=F32
        ).astype(BF)

    jobs = [(h, i) for h in range(STEP_HEADS) for i in range(rows // block)]
    ready = scores_of(*jobs[0])
    waiting = None
    for n, job in enumerate(jobs):
        scores = ready
        if n + 1 < len(jobs):
            ready = scores_of(*jobs[n + 1])
        probs = softmax_of(*job, scores)
        if waiting is not None:
            attend(*waiting)
        waiting = (*job, probs)
    attend(*waiting)


def attend_forward(base, queries, keys, values, ids):
    rows = queries.shape[0]
    head = pl.BlockSpec((rows, DH * STEP_HEADS), lambda i, b: (0, b[0] + i))
    return pl.pallas_call(
        forward_kernel,
        grid_spec=pltpu.PrefetchScalarGridSpec(
            num_scalar_prefetch=1,
            grid=(HALF // STEP_HEADS,),
            in_specs=[head, head, head, pl.BlockSpec((1, rows), lambda i, b: (0, 0))],
            out_specs=[
                pl.BlockSpec((rows, DH * STEP_HEADS), lambda i, b: (0, i)),
                pl.BlockSpec((STEP_HEADS, rows, rows), lambda i, b: (i, 0, 0)),
            ],
            scratch_shapes=[pltpu.VMEM((rows, rows), F32)],
        ),
        out_shape=[
            jax.ShapeDtypeStruct((rows, HALF * DH), BF),
            jax.ShapeDtypeStruct((HALF, rows, rows), BF),
        ],
        compiler_params=grid_params(),
        cost_estimate=pl.CostEstimate(
            flops=FLOPS_6US, bytes_accessed=9 << 20, transcendentals=1 << 20
        ),
        name="attend_forward",
    )(base, queries, keys, values, ids)


def backward_kernel(base, q_ref, k_ref, v_ref, g_ref, att_ref, prob_ref, *refs):
    dq_ref, dk_ref, dv_ref = refs[-3:]
    rows = q_ref.shape[0]
    block = 256
    count = rows // block
    inner, grad_t, query_t, sums = {}, {}, {}, {}

    def cut(h, i):
        return slice(h * DH, (h + 1) * DH), i * block, (i + 1) * block

    def prepare(h):
        cols = cut(h, 0)[0]
        grad = g_ref[:, cols]
        inner[h] = jnp.sum(
            grad.astype(F32) * att_ref[:, cols].astype(F32), axis=1, keepdims=True
        )
        grad_t[h] = grad.T
        query_t[h] = q_ref[:, cols].T
        sums[h] = []

    def grad_probs_of(h, i):
        cols, lo, hi = cut(h, i)
        return lax.dot_general(
            g_ref[lo:hi, cols],
            v_ref[:hi, cols],
            (((1,), (1,)), ((), ())),
            preferred_element_type=F32,
        )

    def grad_scores_of(h, i, grad_probs):
        _, lo, hi = cut(h, i)
        probs = prob_ref[h, lo:hi, :hi].astype(F32)
        return (probs * (grad_probs - inner[h][lo:hi, :])).astype(BF)

    def finish(h, i, grad_scores):
        cols, lo, hi = cut(h, i)
        probs = prob_ref[h, lo:hi, :hi]
        dq_ref[lo:hi, cols] = (
            SCALE * jnp.dot(grad_scores, k_ref[:hi, cols], preferred_element_type=F32)
        ).astype(BF)
        sums[h].append(
            (
                jnp.dot(grad_t[h][:, lo:hi], probs, preferred_element_type=F32),
                jnp.dot(query_t[h][:, lo:hi], grad_scores, preferred_element_type=F32),
            )
        )
        if i < count - 1:
            return
        for n, (out_ref, factor) in enumerate(((dv_ref, 1.0), (dk_ref, SCALE))):
            for j in range(count):
                _, lo, hi = cut(h, j)
                total = sums[h][j][n][:, lo:hi]
                for m in range(j + 1, count):
                    total = total + sums[h][m][n][:, lo:hi]
                out_ref[lo:hi, cols] = (total * factor).astype(BF).T

    jobs = [(h, i) for h in range(STEP_HEADS) for i in range(count)]
    prepare(0)
    ready = grad_probs_of(*jobs[0])
    waiting = None
    for n, job in enumerate(jobs):
        grad_probs = ready
        if n + 1 < len(jobs):
            if jobs[n + 1][1] == 0:
                prepare(jobs[n + 1][0])
            ready = grad_probs_of(*jobs[n + 1])
        grad_scores = grad_scores_of(*job, grad_probs)
        if waiting is not None:
            finish(*waiting)
        waiting = (*job, grad_scores)
    finish(*waiting)


def attend_backward(base, queries, keys, values, grad, attended, probs, previous):
    rows = queries.shape[0]
    head = pl.BlockSpec((rows, DH * STEP_HEADS), lambda i, b: (0, b[0] + i))
    half = pl.BlockSpec((rows, DH * STEP_HEADS), lambda i, b: (0, i))
    shape = jax.ShapeDtypeStruct(queries.shape, BF)
    return pl.pallas_call(
        backward_kernel,
        grid_spec=pltpu.PrefetchScalarGridSpec(
            num_scalar_prefetch=1,
            grid=(HALF // STEP_HEADS,),
            in_specs=[head, head, head, half, half]
            + [pl.BlockSpec((STEP_HEADS, rows, rows), lambda i, b: (i, 0, 0))]
            + [pl.BlockSpec(memory_space=pl.ANY)] * len(previous),
            out_specs=[head, head, head],
        ),
        out_shape=[shape, shape, shape],
        input_output_aliases={7 + n: n for n in range(len(previous))},
        compiler_params=grid_params(),
        cost_estimate=pl.CostEstimate(
            flops=FLOPS_4US, bytes_accessed=12 << 20, transcendentals=0
        ),
        name="attend_backward",
    )(base, queries, keys, values, grad, attended, probs, *previous)


def row_of(coset, other, block):
    core, j, i, z = block % 2, (block // 2) % 2, (block // 4) % 2, block // 8
    odd_x, odd_y = (z + other[0]) % 2, (z + other[1]) % 2
    x = (1 - coset[0] if odd_x else coset[0]) + 2 * i
    y = (1 - coset[1] if odd_y else coset[1]) + 2 * j
    return 16 * (x * 32 + (z % 2) * 16 + (z // 2) * 8 + y * 2 + core)


def coset_parts():
    yield (0, 0), 0, 32
    for other in CLASSES:
        yield other, 0, 16
        yield other, 16, 32


def project_kernel(coset, up_own_ref, up_other_ref, *refs):
    pieces, (own_ref, other_ref, weight_ref) = refs[:7], refs[7:]
    place = (coset[0], coset[1])
    for ref, (other, lo, hi) in zip(pieces, coset_parts()):
        for block in range(lo, hi):
            row = pl.multiple_of(row_of(place, other, block), 16)
            weight_ref[pl.ds(row, 16), :] = ref[16 * (block - lo) : 16 * (block - lo + 1), :]
    step = 512
    for up_ref, out_ref in ((up_other_ref, other_ref), (up_own_ref, own_ref)):
        for lo in range(0, out_ref.shape[1], step):
            out_ref[:, lo : lo + step] = jnp.dot(
                up_ref[...], weight_ref[:, lo : lo + step], preferred_element_type=F32
            ).astype(BF)


SMEM = pl.BlockSpec(memory_space=pltpu.SMEM)
VMEM = pl.BlockSpec(memory_space=pltpu.VMEM)


def project(coset, up_own, up_other, pieces):
    rows, width = up_own.shape
    cols = pieces[0].shape[1]
    return pl.pallas_call(
        project_kernel,
        in_specs=[SMEM] + [VMEM] * (2 + len(pieces)),
        out_specs=[VMEM] * 2,
        out_shape=[jax.ShapeDtypeStruct((rows, cols), BF)] * 2,
        scratch_shapes=[pltpu.VMEM((width, cols), BF)],
        compiler_params=whole_params(20),
        cost_estimate=pl.CostEstimate(
            flops=FLOPS_4US, bytes_accessed=10 << 20, transcendentals=0
        ),
        name="project",
    )(coset, up_own, up_other, *pieces)


def weight_kernel(coset, up_own_ref, up_other_ref, att_own_ref, att_other_ref, *refs):
    outs, sums_ref = refs[:7], refs[7]
    width = up_own_ref.shape[1]
    place = (coset[0], coset[1])
    step, cut = 256, 512

    def strip(lo):
        return jnp.concatenate(
            [up_own_ref[:, lo : lo + step].T, up_other_ref[:, lo : lo + step].T], axis=1
        )

    ready = strip(0)
    for lo in range(0, width, step):
        up_t = ready
        if lo + step < width:
            ready = strip(lo + step)
        for col in range(0, sums_ref.shape[1], cut):
            attended = jnp.concatenate(
                [att_own_ref[:, col : col + cut], att_other_ref[:, col : col + cut]], axis=0
            )
            sums_ref[lo : lo + step, col : col + cut] = jnp.dot(
                up_t, attended, preferred_element_type=F32
            ).astype(BF)
    for ref, (other, lo, hi) in zip(outs, coset_parts()):
        for block in range(lo, hi):
            row = pl.multiple_of(row_of(place, other, block), 16)
            ref[16 * (block - lo) : 16 * (block - lo + 1), :] = sums_ref[pl.ds(row, 16), :]


def weight_sums(coset, up_own, up_other, att_own, att_other):
    width = up_own.shape[1]
    cols = att_own.shape[1]
    sizes = [16 * (hi - lo) for _, lo, hi in coset_parts()]
    return pl.pallas_call(
        weight_kernel,
        in_specs=[SMEM] + [VMEM] * 4,
        out_specs=[VMEM] * len(sizes),
        out_shape=[jax.ShapeDtypeStruct((size, cols), BF) for size in sizes],
        scratch_shapes=[pltpu.VMEM((width, cols), BF)],
        compiler_params=whole_params(20),
        cost_estimate=pl.CostEstimate(
            flops=FLOPS_4US, bytes_accessed=10 << 20, transcendentals=0
        ),
        name="weight_sums",
    )(coset, up_own, up_other, att_own, att_other)


def spread_kernel(weight_ref, out_ref):
    cols = out_ref.shape[2]
    for n in range(out_ref.shape[0]):
        out_ref[n] = weight_ref[:, cols * (n % 2) : cols * (n % 2 + 1)]


def gather_weight(weight):
    rows, cols = weight.shape[0], weight.shape[1] // 2
    pieces = pl.pallas_call(
        spread_kernel,
        in_specs=[VMEM],
        out_specs=VMEM,
        out_shape=jax.ShapeDtypeStruct((32, rows, cols), BF),
        compiler_params=whole_params(8),
        name="spread",
    )(weight)
    return exchange(pieces).reshape(32 * rows, cols)


def gather_cosets(block):
    half = block.shape[0] // 2
    parts = (block[:half], block[half:])
    result = [block]
    for axis in range(3):
        for half in range(2):
            result.append(lax.ppermute(parts[half], "d", shift(axis, 2 * half - 1)))
    return result


def add_kernel(own_ref, *refs):
    received, out_ref = refs[:6], refs[6]
    rows = received[0].shape[0]
    for half in range(2):
        for lo in range(0, rows, 16):
            total = own_ref[rows * half + lo : rows * half + lo + 16, :].astype(F32)
            for axis in range(3):
                total = total + received[2 * axis + half][lo : lo + 16, :].astype(F32)
            out_ref[rows * half + lo : rows * half + lo + 16, :] = total.astype(BF)


def reduce_cosets(pieces):
    received = []
    for n, piece in enumerate(pieces[1:]):
        received.append(lax.ppermute(piece, "d", shift(n // 2, 1 - 2 * (n % 2))))
    return received


def add_received(own, received):
    return pl.pallas_call(
        add_kernel,
        in_specs=[VMEM] * 7,
        out_specs=VMEM,
        out_shape=jax.ShapeDtypeStruct(own.shape, BF),
        compiler_params=whole_params(8),
        cost_estimate=pl.CostEstimate(flops=1 << 28, bytes_accessed=5 << 20, transcendentals=0),
        name="add_received",
    )(own, *received)


def own_rows(rows_in, total_tokens):
    rows = rows_in.reshape(16, 2, *rows_in.shape[1:]).astype(F32)
    sums = jnp.sum(rows, axis=0) * (1.0 / math.sqrt(total_tokens))
    return jnp.concatenate([sums[0], sums[1]], axis=1)


def shards(queries, keys, values, upstream, weight, sample_ids):
    rows = queries.shape[0]
    me = lax.axis_index("d")
    core = jnp.bitwise_and(me, 1)
    z = jnp.bitwise_and(jnp.right_shift(me, 4), 1)
    kx = jnp.bitwise_and(jnp.right_shift(me, 5) + z, 1)
    ky = jnp.bitwise_and(jnp.right_shift(me, 1) + z, 1)
    coset = jnp.stack([kx, ky]).astype(jnp.int32)
    steps = HALF // STEP_HEADS
    base_own = (steps * core).astype(jnp.int32).reshape(1)
    base_other = (steps * (1 - core)).astype(jnp.int32).reshape(1)

    up_other = lax.ppermute(upstream, "d", CORE_SWAP)
    mine = gather_weight(weight)
    att_a, prob_a = attend_forward(base_other, queries, keys, values, sample_ids)
    att_other = lax.ppermute(att_a, "d", CORE_SWAP)
    att_b, prob_b = attend_forward(base_own, queries, keys, values, sample_ids)
    sums = weight_sums(coset, upstream, up_other, att_b, att_other)
    received = reduce_cosets(sums)
    mine, _ = lax.optimization_barrier((mine, sums[0]))
    gathered = gather_cosets(mine)
    reduced = add_received(sums[0], received)
    rows_in = exchange(reduced.reshape(32, -1, reduced.shape[1]))
    grad_own, grad_sent = project(coset, upstream, up_other, gathered)
    grad_other = lax.ppermute(grad_sent, "d", CORE_SWAP)
    outs = attend_backward(base_own, queries, keys, values, grad_own, att_b, prob_b, ())
    outs = attend_backward(
        base_other, queries, keys, values, grad_other, att_a, prob_a, tuple(outs)
    )
    grad_weight = own_rows(rows_in, rows * lax.axis_size("d"))
    return (*outs, grad_weight)


def solution(mesh):
    flat = Mesh(mesh.devices.reshape(-1), ("d",))
    return jax.shard_map(
        shards,
        mesh=flat,
        in_specs=(P("d", None),) * 6,
        out_specs=(P("d", None),) * 4,
        check_vma=False,
    )
```

```python
import math

import jax
import jax.numpy as jnp
from jax import lax
from jax.experimental import pallas as pl
from jax.experimental.pallas import tpu as pltpu
from jax.sharding import Mesh
from jax.sharding import PartitionSpec as P


DH = 128
HALF = 8
LIMIT = 58
LIMIT_PROJECT = 50
FLOPS_4US = 2 << 30
FLOPS_6US = 3 << 30
SCALE = 1.0 / math.sqrt(DH)
LOG2E = math.log2(math.e)
BF = jnp.bfloat16
F32 = jnp.float32
CLASSES = ((1, 0), (0, 1), (1, 1))


def coords(i):
    return (i // 32, (i // 2) % 4, 2 * ((i // 8) % 2) + (i // 16) % 2, i % 2)


def device_at(x, y, z, core):
    x, y, z = x % 4, y % 4, z % 4
    return x * 32 + (z % 2) * 16 + (z // 2) * 8 + y * 2 + core


COSETS = [
    [
        device_at((kx + z) % 2 + 2 * i, (ky + z) % 2 + 2 * j, z, core)
        for z in range(4)
        for i in range(2)
        for j in range(2)
        for core in range(2)
    ]
    for kx in range(2)
    for ky in range(2)
]
CORE_SWAP = [(i, i ^ 1) for i in range(128)]


def shift(axis, by):
    pairs = []
    for i in range(128):
        place = list(coords(i))
        place[axis] += by
        pairs.append((i, device_at(*place)))
    return pairs


def exchange(pieces):
    return lax.all_to_all(pieces, "d", 0, 0, axis_index_groups=COSETS, tiled=True)


SMEM = pl.BlockSpec(memory_space=pltpu.SMEM)
VMEM = pl.BlockSpec(memory_space=pltpu.VMEM)
HBM = pl.BlockSpec(memory_space=pltpu.HBM)


def whole_params(mib):
    return pltpu.CompilerParams(vmem_limit_bytes=mib * 1024 * 1024)


BLOCK = 256
PACKED = 3 * BLOCK
CHUNK = 2


def places(h, i):
    cols = slice(h * DH, (h + 1) * DH)
    packed = slice(0, BLOCK) if i == 0 else slice(BLOCK, PACKED)
    return cols, i * BLOCK, (i + 1) * BLOCK, packed


def chunk_copy(source, base, buffer, sem, n, chunk):
    wide = CHUNK * DH
    start = pl.multiple_of(base * (HALF * DH) + chunk * wide, DH)
    return pltpu.make_async_copy(
        source.at[:, pl.ds(start, wide)],
        buffer.at[:, chunk * wide : (chunk + 1) * wide],
        sem.at[n, chunk],
    )


def forward_kernel(base_ref, ids_ref, q_hbm, k_hbm, v_hbm, att_hbm, prob_hbm, *scratch):
    q_ref, k_ref, v_ref, att_ref, prob_ref, bias_ref, in_sem, prob_sem, att_sem = scratch
    rows = q_ref.shape[0]
    base = base_ref[0]
    loads = [
        [
            chunk_copy(source, base, buffer, in_sem, n, chunk)
            for n, (source, buffer) in enumerate(((q_hbm, q_ref), (k_hbm, k_ref), (v_hbm, v_ref)))
        ]
        for chunk in range(HALF // CHUNK)
    ]
    for group in loads:
        for copy in group:
            copy.start()

    t = lax.broadcasted_iota(jnp.int32, (rows, rows), 0)
    u = lax.broadcasted_iota(jnp.int32, (rows, rows), 1)
    ids = ids_ref[...].astype(F32)
    own = jnp.broadcast_to(ids, (DH, rows)).T[:, :1]
    bias_ref[...] = jnp.where(jnp.logical_and(u <= t, own == ids), 0.0, -1e30)

    def scores_of(h, i):
        cols, lo, hi, _ = places(h, i)
        if i == 0 and h % CHUNK == 0:
            for copy in loads[h // CHUNK]:
                copy.wait()
        return lax.dot_general(
            q_ref[lo:hi, cols],
            k_ref[:hi, cols],
            (((1,), (1,)), ((), ())),
            preferred_element_type=F32,
        )

    stores = [
        pltpu.make_async_copy(prob_ref.at[h], prob_hbm.at[h], prob_sem.at[h]) for h in range(HALF)
    ]

    def softmax_of(h, i, scores):
        _, lo, hi, packed = places(h, i)
        scores = scores * (SCALE * LOG2E) + bias_ref[lo:hi, :hi]
        raised = jnp.exp2(scores - jnp.max(scores, axis=1, keepdims=True))
        total = jnp.sum(raised, axis=1, keepdims=True)
        probs = (raised * (1.0 / total)).astype(BF)
        prob_ref[h, :, packed] = probs
        return probs

    def attend(h, i, probs):
        cols, lo, hi, _ = places(h, i)
        att_ref[lo:hi, cols] = jnp.dot(
            probs, v_ref[:hi, cols], preferred_element_type=F32
        ).astype(BF)

    jobs = [(h, i) for h in range(HALF) for i in range(rows // BLOCK)]
    ready = scores_of(*jobs[0])
    waiting = None
    for n, job in enumerate(jobs):
        scores = ready
        if n + 1 < len(jobs):
            ready = scores_of(*jobs[n + 1])
        probs = softmax_of(*job, scores)
        if waiting is not None:
            attend(*waiting)
        waiting = (*job, probs)
        if job[1] == 1:
            stores[job[0]].start()
    attend(*waiting)
    keep = pltpu.make_async_copy(att_ref, att_hbm, att_sem)
    keep.start()
    for copy in stores:
        copy.wait()
    keep.wait()


def attend_forward(base, queries, keys, values, ids):
    rows = queries.shape[0]
    cols = HALF * DH
    return pl.pallas_call(
        forward_kernel,
        in_specs=[SMEM, VMEM, HBM, HBM, HBM],
        out_specs=[HBM, HBM],
        out_shape=[
            jax.ShapeDtypeStruct((rows, cols), BF),
            jax.ShapeDtypeStruct((HALF, BLOCK, PACKED), BF),
        ],
        scratch_shapes=[pltpu.VMEM((rows, cols), BF)] * 4
        + [
            pltpu.VMEM((HALF, BLOCK, PACKED), BF),
            pltpu.VMEM((rows, rows), F32),
            pltpu.SemaphoreType.DMA((3, HALF // CHUNK)),
            pltpu.SemaphoreType.DMA((HALF,)),
            pltpu.SemaphoreType.DMA,
        ],
        compiler_params=whole_params(LIMIT),
        cost_estimate=pl.CostEstimate(
            flops=FLOPS_6US, bytes_accessed=9 << 20, transcendentals=1 << 20
        ),
        name="attend_forward",
    )(base, ids, queries, keys, values)


def backward_kernel(base_ref, g_ref, q_hbm, k_hbm, v_hbm, att_hbm, prob_hbm, *refs):
    dq_hbm, dk_hbm, dv_hbm = refs[-13:-10]
    q_ref, k_ref, v_ref, att_ref, prob_ref, dq_ref, dk_ref, dv_ref = refs[-10:-2]
    in_sem, out_sem = refs[-2:]
    rows = q_ref.shape[0]
    base = base_ref[0]
    count = rows // BLOCK
    loads = []
    for chunk in range(HALF // CHUNK):
        group = [
            chunk_copy(source, base, buffer, in_sem, n, chunk)
            for n, (source, buffer) in enumerate(((q_hbm, q_ref), (k_hbm, k_ref), (v_hbm, v_ref)))
        ]
        group.append(chunk_copy(att_hbm, 0, att_ref, in_sem, 3, chunk))
        heads = slice(chunk * CHUNK, (chunk + 1) * CHUNK)
        group.append(
            pltpu.make_async_copy(prob_hbm.at[heads], prob_ref.at[heads], in_sem.at[4, chunk])
        )
        loads.append(group)
    for group in loads:
        for copy in group:
            copy.start()
    wide = CHUNK * DH
    stores = [
        [
            pltpu.make_async_copy(
                buffer.at[:, chunk * wide : (chunk + 1) * wide],
                target.at[
                    :, pl.ds(pl.multiple_of(base * (HALF * DH) + chunk * wide, DH), wide)
                ],
                out_sem.at[n, chunk],
            )
            for n, (buffer, target) in enumerate(
                ((dq_ref, dq_hbm), (dk_ref, dk_hbm), (dv_ref, dv_hbm))
            )
        ]
        for chunk in range(HALF // CHUNK)
    ]
    inner, grad_t, query_t, sums = {}, {}, {}, {}

    def prepare(h):
        cols = places(h, 0)[0]
        if h % CHUNK == 0:
            for copy in loads[h // CHUNK]:
                copy.wait()
        grad = g_ref[:, cols]
        inner[h] = jnp.sum(
            grad.astype(F32) * att_ref[:, cols].astype(F32), axis=1, keepdims=True
        )
        grad_t[h] = grad.T
        query_t[h] = q_ref[:, cols].T
        sums[h] = []

    def grad_probs_of(h, i):
        cols, lo, hi, _ = places(h, i)
        return lax.dot_general(
            g_ref[lo:hi, cols],
            v_ref[:hi, cols],
            (((1,), (1,)), ((), ())),
            preferred_element_type=F32,
        )

    def grad_scores_of(h, i, grad_probs):
        _, lo, hi, packed = places(h, i)
        probs = prob_ref[h, :, packed].astype(F32)
        return (probs * (grad_probs - inner[h][lo:hi, :])).astype(BF)

    def finish(h, i, grad_scores):
        cols, lo, hi, packed = places(h, i)
        probs = prob_ref[h, :, packed]
        dq_ref[lo:hi, cols] = (
            SCALE * jnp.dot(grad_scores, k_ref[:hi, cols], preferred_element_type=F32)
        ).astype(BF)
        sums[h].append(
            (
                jnp.dot(grad_t[h][:, lo:hi], probs, preferred_element_type=F32),
                jnp.dot(query_t[h][:, lo:hi], grad_scores, preferred_element_type=F32),
            )
        )
        if i < count - 1:
            return
        for n, (out_ref, factor) in enumerate(((dv_ref, 1.0), (dk_ref, SCALE))):
            for j in range(count):
                _, lo, hi, _ = places(h, j)
                total = sums[h][j][n][:, lo:hi]
                for m in range(j + 1, count):
                    total = total + sums[h][m][n][:, lo:hi]
                out_ref[lo:hi, cols] = (total * factor).astype(BF).T
        if h % CHUNK == CHUNK - 1:
            for copy in stores[h // CHUNK]:
                copy.start()

    jobs = [(h, i) for h in range(HALF) for i in range(count)]
    prepare(0)
    ready = grad_probs_of(*jobs[0])
    waiting = None
    for n, job in enumerate(jobs):
        grad_probs = ready
        if n + 1 < len(jobs):
            if jobs[n + 1][1] == 0:
                prepare(jobs[n + 1][0])
            ready = grad_probs_of(*jobs[n + 1])
        grad_scores = grad_scores_of(*job, grad_probs)
        if waiting is not None:
            finish(*waiting)
        waiting = (*job, grad_scores)
    finish(*waiting)
    for group in stores:
        for copy in group:
            copy.wait()


def attend_backward(base, queries, keys, values, grad, attended, probs, previous):
    rows = queries.shape[0]
    cols = HALF * DH
    shape = jax.ShapeDtypeStruct(queries.shape, BF)
    chunks = HALF // CHUNK
    half = pltpu.VMEM((rows, cols), BF)
    return pl.pallas_call(
        backward_kernel,
        in_specs=[SMEM, VMEM] + [HBM] * (5 + len(previous)),
        out_specs=[HBM] * 3,
        out_shape=[shape, shape, shape],
        scratch_shapes=[half] * 4
        + [pltpu.VMEM((HALF, BLOCK, PACKED), BF)]
        + [half] * 3
        + [pltpu.SemaphoreType.DMA((5, chunks)), pltpu.SemaphoreType.DMA((3, chunks))],
        input_output_aliases={7 + n: n for n in range(len(previous))},
        compiler_params=whole_params(LIMIT),
        cost_estimate=pl.CostEstimate(
            flops=FLOPS_4US, bytes_accessed=12 << 20, transcendentals=0
        ),
        name="attend_backward",
    )(base, grad, queries, keys, values, attended, probs, *previous)


def row_of(coset, other, block):
    core, j, i, z = block % 2, (block // 2) % 2, (block // 4) % 2, block // 8
    odd_x, odd_y = (z + other[0]) % 2, (z + other[1]) % 2
    x = (1 - coset[0] if odd_x else coset[0]) + 2 * i
    y = (1 - coset[1] if odd_y else coset[1]) + 2 * j
    return 16 * (x * 32 + (z % 2) * 16 + (z // 2) * 8 + y * 2 + core)


def coset_parts():
    yield (0, 0), 0, 32
    for other in CLASSES:
        yield other, 0, 16
        yield other, 16, 32


def project_kernel(coset, up_own_hbm, up_other_hbm, *refs):
    pieces, (own_hbm, other_hbm) = refs[:7], refs[7:9]
    weight_ref, up_ref, out_ref, up_sem, out_sem = refs[9:]
    cols = weight_ref.shape[1]
    place = (coset[0], coset[1])
    ups = []
    for n, source in enumerate((up_other_hbm, up_own_hbm)):
        ups.append(pltpu.make_async_copy(source, up_ref.at[n], up_sem.at[n]))
        ups[n].start()
    for piece, (other, lo, hi) in zip(pieces, coset_parts()):
        for block in range(lo, hi):
            row = pl.multiple_of(row_of(place, other, block), 16)
            weight_ref[pl.ds(row, 16), :] = piece[16 * (block - lo) : 16 * (block - lo + 1), :]
    step = 512
    stores = []
    for n, target in enumerate((other_hbm, own_hbm)):
        ups[n].wait()
        for lo in range(0, cols, step):
            out_ref[n, :, lo : lo + step] = jnp.dot(
                up_ref[n], weight_ref[:, lo : lo + step], preferred_element_type=F32
            ).astype(BF)
        stores.append(pltpu.make_async_copy(out_ref.at[n], target, out_sem.at[n]))
        stores[n].start()
    for copy in stores:
        copy.wait()


def project(coset, up_own, up_other, pieces):
    rows, width = up_own.shape
    cols = pieces[0].shape[1]
    return pl.pallas_call(
        project_kernel,
        in_specs=[SMEM, HBM, HBM] + [VMEM] * len(pieces),
        out_specs=[HBM] * 2,
        out_shape=[jax.ShapeDtypeStruct((rows, cols), BF)] * 2,
        scratch_shapes=[
            pltpu.VMEM((width, cols), BF),
            pltpu.VMEM((2, rows, width), BF),
            pltpu.VMEM((2, rows, cols), BF),
            pltpu.SemaphoreType.DMA((2,)),
            pltpu.SemaphoreType.DMA((2,)),
        ],
        compiler_params=whole_params(LIMIT_PROJECT),
        cost_estimate=pl.CostEstimate(
            flops=FLOPS_4US, bytes_accessed=10 << 20, transcendentals=0
        ),
        name="project",
    )(coset, up_own, up_other, *pieces)


def weight_kernel(coset, up_other_ref, up_own_hbm, att_own_hbm, att_other_hbm, *refs):
    outs, stages = refs[:7], refs[7:14]
    up_ref, att_ref, up_t_ref, first_ref, second_ref, up_sem, att_sem, out_sem = refs[14:]
    rows, width = up_own_hbm.shape
    place = (coset[0], coset[1])
    step, cut = 256, 512
    att_loads, up_loads = [], []
    for col in range(2):
        att_loads.append(
            [
                pltpu.make_async_copy(
                    source.at[:, col * cut : (col + 1) * cut],
                    att_ref.at[n * rows : (n + 1) * rows, col * cut : (col + 1) * cut],
                    att_sem.at[n, col],
                )
                for n, source in enumerate((att_own_hbm, att_other_hbm))
            ]
        )
    for m in range(width // step):
        up_loads.append(
            pltpu.make_async_copy(
                up_own_hbm.at[:, m * step : (m + 1) * step],
                up_ref.at[:, m * step : (m + 1) * step],
                up_sem.at[m],
            )
        )
    for copy in [*att_loads[0], *up_loads, *att_loads[1]]:
        copy.start()

    def turn(m):
        up_loads[m].wait()
        strip = slice(m * step, (m + 1) * step)
        for n, source in enumerate((up_ref, up_other_ref)):
            up_t_ref[strip, n * rows : (n + 1) * rows] = source[:, strip].T

    turn(0)
    stores = []
    for col, sums_ref in enumerate((first_ref, second_ref)):
        for copy in att_loads[col]:
            copy.wait()
        cols = slice(col * cut, (col + 1) * cut)
        for m in range(width // step):
            if col == 0 and (m + 1) * step < width:
                turn(m + 1)
            sums_ref[m * step : (m + 1) * step, :] = jnp.dot(
                up_t_ref[m * step : (m + 1) * step, :],
                att_ref[:, cols],
                preferred_element_type=F32,
            ).astype(BF)
        for k, (out, stage, (other, lo, hi)) in enumerate(zip(outs, stages, coset_parts())):
            for block in range(lo, hi):
                row = pl.multiple_of(row_of(place, other, block), 16)
                stage[col, 16 * (block - lo) : 16 * (block - lo + 1), :] = sums_ref[
                    pl.ds(row, 16), :
                ]
            copy = pltpu.make_async_copy(stage.at[col], out.at[:, cols], out_sem.at[col, k])
            copy.start()
            stores.append(copy)
    for copy in stores:
        copy.wait()


def weight_sums(coset, up_own, up_other, att_own, att_other):
    rows, width = up_own.shape
    cols = att_own.shape[1]
    sizes = [16 * (hi - lo) for _, lo, hi in coset_parts()]
    return pl.pallas_call(
        weight_kernel,
        in_specs=[SMEM, VMEM] + [HBM] * 3,
        out_specs=[HBM] * len(sizes),
        out_shape=[jax.ShapeDtypeStruct((size, cols), BF) for size in sizes],
        scratch_shapes=[pltpu.VMEM((2, size, cols // 2), BF) for size in sizes]
        + [
            pltpu.VMEM((rows, width), BF),
            pltpu.VMEM((2 * rows, cols), BF),
            pltpu.VMEM((width, 2 * rows), BF),
            pltpu.VMEM((width, cols // 2), BF),
            pltpu.VMEM((width, cols // 2), BF),
            pltpu.SemaphoreType.DMA((width // 256,)),
            pltpu.SemaphoreType.DMA((2, 2)),
            pltpu.SemaphoreType.DMA((2, len(sizes))),
        ],
        compiler_params=whole_params(LIMIT),
        cost_estimate=pl.CostEstimate(
            flops=FLOPS_4US, bytes_accessed=10 << 20, transcendentals=0
        ),
        name="weight_sums",
    )(coset, up_other, up_own, att_own, att_other)


def spread_kernel(weight_ref, out_hbm, sem):
    cols = out_hbm.shape[2]
    copies = [
        pltpu.make_async_copy(
            weight_ref.at[:, cols * (n % 2) : cols * (n % 2 + 1)], out_hbm.at[n], sem.at[n]
        )
        for n in range(out_hbm.shape[0])
    ]
    for copy in copies:
        copy.start()
    for copy in copies:
        copy.wait()


def gather_weight(weight):
    rows, cols = weight.shape[0], weight.shape[1] // 2
    pieces = pl.pallas_call(
        spread_kernel,
        in_specs=[VMEM],
        out_specs=HBM,
        out_shape=jax.ShapeDtypeStruct((32, rows, cols), BF),
        scratch_shapes=[pltpu.SemaphoreType.DMA((32,))],
        compiler_params=whole_params(LIMIT),
        name="spread",
    )(weight)
    return exchange(pieces).reshape(32 * rows, cols)


def gather_cosets(block):
    half = block.shape[0] // 2
    parts = (block[:half], block[half:])
    result = [block]
    for axis in range(3):
        for half in range(2):
            result.append(lax.ppermute(parts[half], "d", shift(axis, 2 * half - 1)))
    return result


def add_kernel(own_ref, *refs):
    received, out_ref = refs[:6], refs[6]
    rows = received[0].shape[0]
    for half in range(2):
        for lo in range(0, rows, 16):
            total = own_ref[rows * half + lo : rows * half + lo + 16, :].astype(F32)
            for axis in range(3):
                total = total + received[2 * axis + half][lo : lo + 16, :].astype(F32)
            out_ref[rows * half + lo : rows * half + lo + 16, :] = total.astype(BF)


def reduce_cosets(pieces):
    received = []
    for n, piece in enumerate(pieces[1:]):
        received.append(lax.ppermute(piece, "d", shift(n // 2, 1 - 2 * (n % 2))))
    return received


def add_received(own, received):
    return pl.pallas_call(
        add_kernel,
        in_specs=[VMEM] * 7,
        out_specs=VMEM,
        out_shape=jax.ShapeDtypeStruct(own.shape, BF),
        compiler_params=whole_params(8),
        cost_estimate=pl.CostEstimate(flops=1 << 28, bytes_accessed=5 << 20, transcendentals=0),
        name="add_received",
    )(own, *received)


def own_rows(rows_in, total_tokens):
    rows = rows_in.reshape(16, 2, *rows_in.shape[1:]).astype(F32)
    sums = jnp.sum(rows, axis=0) * (1.0 / math.sqrt(total_tokens))
    return jnp.concatenate([sums[0], sums[1]], axis=1)


def shards(queries, keys, values, upstream, weight, sample_ids):
    rows = queries.shape[0]
    me = lax.axis_index("d")
    core = jnp.bitwise_and(me, 1)
    z = jnp.bitwise_and(jnp.right_shift(me, 4), 1)
    kx = jnp.bitwise_and(jnp.right_shift(me, 5) + z, 1)
    ky = jnp.bitwise_and(jnp.right_shift(me, 1) + z, 1)
    coset = jnp.stack([kx, ky]).astype(jnp.int32)
    base_own = core.astype(jnp.int32).reshape(1)
    base_other = (1 - core).astype(jnp.int32).reshape(1)

    up_other = lax.ppermute(upstream, "d", CORE_SWAP)
    mine = gather_weight(weight)
    att_a, prob_a = attend_forward(base_other, queries, keys, values, sample_ids)
    att_other = lax.ppermute(att_a, "d", CORE_SWAP)
    att_b, prob_b = attend_forward(base_own, queries, keys, values, sample_ids)
    sums = weight_sums(coset, upstream, up_other, att_b, att_other)
    received = reduce_cosets(sums)
    mine, _ = lax.optimization_barrier((mine, sums[0]))
    gathered = gather_cosets(mine)
    reduced = add_received(sums[0], received)
    rows_in = exchange(reduced.reshape(32, -1, reduced.shape[1]))
    grad_own, grad_sent = project(coset, upstream, up_other, gathered)
    grad_other = lax.ppermute(grad_sent, "d", CORE_SWAP)
    outs = attend_backward(
        base_own, queries, keys, values, grad_own, att_b, prob_b, ()
    )
    outs = attend_backward(
        base_other, queries, keys, values, grad_other, att_a, prob_a, tuple(outs)
    )
    grad_weight = own_rows(rows_in, rows * lax.axis_size("d"))
    return (*outs, grad_weight)


def solution(mesh):
    flat = Mesh(mesh.devices.reshape(-1), ("d",))
    return jax.shard_map(
        shards,
        mesh=flat,
        in_specs=(P("d", None),) * 6,
        out_specs=(P("d", None),) * 4,
        check_vma=False,
    )
```

```python
import functools
import math

import jax
import jax.numpy as jnp
from jax import lax
from jax.experimental import pallas as pl
from jax.experimental.pallas import tpu as pltpu
from jax.sharding import Mesh
from jax.sharding import PartitionSpec as P


DH = 128
HALF = 8
STEP_HEADS = 4
LIMIT = 50
LIMIT_A = 60
LIMIT_BACK = 50
LIMIT_LAST = 50
LIMIT_SPREAD = 58
LIMIT_WHOLE = 20
LIMIT_SMALL = 8
FLOPS_4US = 2 << 30
FLOPS_6US = 3 << 30
SCALE = 1.0 / math.sqrt(DH)
LOG2E = math.log2(math.e)
BF = jnp.bfloat16
F32 = jnp.float32
CLASSES = ((1, 0), (0, 1), (1, 1))


def coords(i):
    return (i // 32, (i // 2) % 4, 2 * ((i // 8) % 2) + (i // 16) % 2, i % 2)


def device_at(x, y, z, core):
    x, y, z = x % 4, y % 4, z % 4
    return x * 32 + (z % 2) * 16 + (z // 2) * 8 + y * 2 + core


COSETS = [
    [
        device_at((kx + z) % 2 + 2 * i, (ky + z) % 2 + 2 * j, z, core)
        for z in range(4)
        for i in range(2)
        for j in range(2)
        for core in range(2)
    ]
    for kx in range(2)
    for ky in range(2)
]
CHIPS = [coset[core::2] for coset in COSETS for core in range(2)]
CORE_SWAP = [(i, i ^ 1) for i in range(128)]


def shift(axis, by):
    pairs = []
    for i in range(128):
        place = list(coords(i))
        place[axis] += by
        pairs.append((i, device_at(*place)))
    return pairs


def exchange(pieces):
    return lax.all_to_all(pieces, "d", 0, 0, axis_index_groups=COSETS, tiled=True)


def grid_params(mib):
    return pltpu.CompilerParams(
        dimension_semantics=("arbitrary",), vmem_limit_bytes=mib * 1024 * 1024
    )


def whole_params(mib):
    return pltpu.CompilerParams(vmem_limit_bytes=mib * 1024 * 1024)


def forward_kernel(base, q_ref, k_ref, v_ref, ids_ref, att_ref, prob_ref, bias_ref):
    rows = q_ref.shape[0]

    @pl.when(pl.program_id(0) == 0)
    def _():
        t = lax.broadcasted_iota(jnp.int32, (rows, rows), 0)
        u = lax.broadcasted_iota(jnp.int32, (rows, rows), 1)
        ids = ids_ref[...].astype(F32)
        own = jnp.broadcast_to(ids, (DH, rows)).T[:, :1]
        bias_ref[...] = jnp.where(jnp.logical_and(u <= t, own == ids), 0.0, -1e30)

    block = 256

    def cut(h, i):
        return slice(h * DH, (h + 1) * DH), i * block, (i + 1) * block

    def scores_of(h, i):
        cols, lo, hi = cut(h, i)
        return lax.dot_general(
            q_ref[lo:hi, cols],
            k_ref[:hi, cols],
            (((1,), (1,)), ((), ())),
            preferred_element_type=F32,
        )

    def softmax_of(h, i, scores):
        _, lo, hi = cut(h, i)
        scores = scores * (SCALE * LOG2E) + bias_ref[lo:hi, :hi]
        raised = jnp.exp2(scores - jnp.max(scores, axis=1, keepdims=True))
        total = jnp.sum(raised, axis=1, keepdims=True)
        probs = (raised * (1.0 / total)).astype(BF)
        prob_ref[h, lo:hi, :hi] = probs
        return probs

    def attend(h, i, probs):
        cols, lo, hi = cut(h, i)
        att_ref[lo:hi, cols] = jnp.dot(
            probs, v_ref[:hi, cols], preferred_element_type=F32
        ).astype(BF)

    jobs = [(h, i) for h in range(STEP_HEADS) for i in range(rows // block)]
    ready = scores_of(*jobs[0])
    waiting = None
    for n, job in enumerate(jobs):
        scores = ready
        if n + 1 < len(jobs):
            ready = scores_of(*jobs[n + 1])
        probs = softmax_of(*job, scores)
        if waiting is not None:
            attend(*waiting)
        waiting = (*job, probs)
    attend(*waiting)


def attend_forward(base, queries, keys, values, ids, mib):
    rows = queries.shape[0]
    head = pl.BlockSpec((rows, DH * STEP_HEADS), lambda i, b: (0, b[0] + i))
    return pl.pallas_call(
        forward_kernel,
        grid_spec=pltpu.PrefetchScalarGridSpec(
            num_scalar_prefetch=1,
            grid=(HALF // STEP_HEADS,),
            in_specs=[head, head, head, pl.BlockSpec((1, rows), lambda i, b: (0, 0))],
            out_specs=[
                pl.BlockSpec((rows, DH * STEP_HEADS), lambda i, b: (0, i)),
                pl.BlockSpec((STEP_HEADS, rows, rows), lambda i, b: (i, 0, 0)),
            ],
            scratch_shapes=[pltpu.VMEM((rows, rows), F32)],
        ),
        out_shape=[
            jax.ShapeDtypeStruct((rows, HALF * DH), BF),
            jax.ShapeDtypeStruct((HALF, rows, rows), BF),
        ],
        compiler_params=grid_params(mib),
        cost_estimate=pl.CostEstimate(
            flops=FLOPS_6US, bytes_accessed=9 << 20, transcendentals=1 << 20
        ),
        name="attend_forward",
    )(base, queries, keys, values, ids)


def backward_kernel(base, q_ref, k_ref, v_ref, g_ref, att_ref, prob_ref, *refs):
    dq_ref, dk_ref, dv_ref = refs[-3:]
    rows = q_ref.shape[0]
    block = 256
    count = rows // block
    inner, grad_t, query_t, sums = {}, {}, {}, {}

    def cut(h, i):
        return slice(h * DH, (h + 1) * DH), i * block, (i + 1) * block

    def prepare(h):
        cols = cut(h, 0)[0]
        grad = g_ref[:, cols]
        inner[h] = jnp.sum(
            grad.astype(F32) * att_ref[:, cols].astype(F32), axis=1, keepdims=True
        )
        grad_t[h] = grad.T
        query_t[h] = q_ref[:, cols].T
        sums[h] = []

    def grad_probs_of(h, i):
        cols, lo, hi = cut(h, i)
        return lax.dot_general(
            g_ref[lo:hi, cols],
            v_ref[:hi, cols],
            (((1,), (1,)), ((), ())),
            preferred_element_type=F32,
        )

    def grad_scores_of(h, i, grad_probs):
        _, lo, hi = cut(h, i)
        probs = prob_ref[h, lo:hi, :hi].astype(F32)
        return (probs * (grad_probs - inner[h][lo:hi, :])).astype(BF)

    def finish(h, i, grad_scores):
        cols, lo, hi = cut(h, i)
        probs = prob_ref[h, lo:hi, :hi]
        dq_ref[lo:hi, cols] = (
            SCALE * jnp.dot(grad_scores, k_ref[:hi, cols], preferred_element_type=F32)
        ).astype(BF)
        sums[h].append(
            (
                jnp.dot(grad_t[h][:, lo:hi], probs, preferred_element_type=F32),
                jnp.dot(query_t[h][:, lo:hi], grad_scores, preferred_element_type=F32),
            )
        )
        if i < count - 1:
            return
        for n, (out_ref, factor) in enumerate(((dv_ref, 1.0), (dk_ref, SCALE))):
            for j in range(count):
                _, lo, hi = cut(h, j)
                total = sums[h][j][n][:, lo:hi]
                for m in range(j + 1, count):
                    total = total + sums[h][m][n][:, lo:hi]
                out_ref[lo:hi, cols] = (total * factor).astype(BF).T

    jobs = [(h, i) for h in range(STEP_HEADS) for i in range(count)]
    prepare(0)
    ready = grad_probs_of(*jobs[0])
    waiting = None
    for n, job in enumerate(jobs):
        grad_probs = ready
        if n + 1 < len(jobs):
            if jobs[n + 1][1] == 0:
                prepare(jobs[n + 1][0])
            ready = grad_probs_of(*jobs[n + 1])
        grad_scores = grad_scores_of(*job, grad_probs)
        if waiting is not None:
            finish(*waiting)
        waiting = (*job, grad_scores)
    finish(*waiting)


def attend_backward(base, queries, keys, values, grad, attended, probs, previous, mib):
    rows = queries.shape[0]
    head = pl.BlockSpec((rows, DH * STEP_HEADS), lambda i, b: (0, b[0] + i))
    half = pl.BlockSpec((rows, DH * STEP_HEADS), lambda i, b: (0, i))
    shape = jax.ShapeDtypeStruct(queries.shape, BF)
    return pl.pallas_call(
        backward_kernel,
        grid_spec=pltpu.PrefetchScalarGridSpec(
            num_scalar_prefetch=1,
            grid=(HALF // STEP_HEADS,),
            in_specs=[head, head, head, half, half]
            + [pl.BlockSpec((STEP_HEADS, rows, rows), lambda i, b: (i, 0, 0))]
            + [pl.BlockSpec(memory_space=pl.ANY)] * len(previous),
            out_specs=[head, head, head],
        ),
        out_shape=[shape, shape, shape],
        input_output_aliases={7 + n: n for n in range(len(previous))},
        compiler_params=grid_params(mib),
        cost_estimate=pl.CostEstimate(
            flops=FLOPS_4US, bytes_accessed=12 << 20, transcendentals=0
        ),
        name="attend_backward",
    )(base, queries, keys, values, grad, attended, probs, *previous)


def row_of(coset, other, block):
    core, j, i, z = block % 2, (block // 2) % 2, (block // 4) % 2, block // 8
    odd_x, odd_y = (z + other[0]) % 2, (z + other[1]) % 2
    x = (1 - coset[0] if odd_x else coset[0]) + 2 * i
    y = (1 - coset[1] if odd_y else coset[1]) + 2 * j
    return 16 * (x * 32 + (z % 2) * 16 + (z // 2) * 8 + y * 2 + core)


def coset_parts():
    yield (0, 0), 0, 32
    for other in CLASSES:
        yield other, 0, 16
        yield other, 16, 32


def project_kernel(kx_ref, ky_ref, up_own_ref, up_other_ref, *refs):
    pieces, (own_ref, other_ref, weight_ref) = refs[:7], refs[7:]
    place = (kx_ref[0], ky_ref[0])
    for ref, (other, lo, hi) in zip(pieces, coset_parts()):
        for block in range(lo, hi):
            row = pl.multiple_of(row_of(place, other, block), 16)
            weight_ref[pl.ds(row, 16), :] = ref[16 * (block - lo) : 16 * (block - lo + 1), :]
    step = 512
    for up_ref, out_ref in ((up_other_ref, other_ref), (up_own_ref, own_ref)):
        for lo in range(0, out_ref.shape[1], step):
            out_ref[:, lo : lo + step] = jnp.dot(
                up_ref[...], weight_ref[:, lo : lo + step], preferred_element_type=F32
            ).astype(BF)


SMEM = pl.BlockSpec(memory_space=pltpu.SMEM)
VMEM = pl.BlockSpec(memory_space=pltpu.VMEM)


def project(coset, up_own, up_other, pieces):
    rows, width = up_own.shape
    cols = pieces[0].shape[1]
    return pl.pallas_call(
        project_kernel,
        in_specs=[SMEM] * 2 + [VMEM] * (2 + len(pieces)),
        out_specs=[VMEM] * 2,
        out_shape=[jax.ShapeDtypeStruct((rows, cols), BF)] * 2,
        scratch_shapes=[pltpu.VMEM((width, cols), BF)],
        compiler_params=whole_params(LIMIT_WHOLE),
        cost_estimate=pl.CostEstimate(
            flops=FLOPS_4US, bytes_accessed=10 << 20, transcendentals=0
        ),
        name="project",
    )(*coset, up_own, up_other, *pieces)


def weight_kernel(kx_ref, ky_ref, up_own_ref, up_other_ref, att_own_ref, att_other_ref, *refs):
    outs, sums_ref = refs[:7], refs[7]
    width = up_own_ref.shape[1]
    place = (kx_ref[0], ky_ref[0])
    step, cut = 256, 512

    def strip(lo):
        return jnp.concatenate(
            [up_own_ref[:, lo : lo + step].T, up_other_ref[:, lo : lo + step].T], axis=1
        )

    ready = strip(0)
    for lo in range(0, width, step):
        up_t = ready
        if lo + step < width:
            ready = strip(lo + step)
        for col in range(0, sums_ref.shape[1], cut):
            attended = jnp.concatenate(
                [att_own_ref[:, col : col + cut], att_other_ref[:, col : col + cut]], axis=0
            )
            sums_ref[lo : lo + step, col : col + cut] = jnp.dot(
                up_t, attended, preferred_element_type=F32
            ).astype(BF)
    for ref, (other, lo, hi) in zip(outs, coset_parts()):
        for block in range(lo, hi):
            row = pl.multiple_of(row_of(place, other, block), 16)
            ref[16 * (block - lo) : 16 * (block - lo + 1), :] = sums_ref[pl.ds(row, 16), :]


def weight_sums(coset, up_own, up_other, att_own, att_other):
    width = up_own.shape[1]
    cols = att_own.shape[1]
    sizes = [16 * (hi - lo) for _, lo, hi in coset_parts()]
    return pl.pallas_call(
        weight_kernel,
        in_specs=[SMEM] * 2 + [VMEM] * 4,
        out_specs=[VMEM] * len(sizes),
        out_shape=[jax.ShapeDtypeStruct((size, cols), BF) for size in sizes],
        scratch_shapes=[pltpu.VMEM((width, cols), BF)],
        compiler_params=whole_params(LIMIT_WHOLE),
        cost_estimate=pl.CostEstimate(
            flops=FLOPS_4US, bytes_accessed=10 << 20, transcendentals=0
        ),
        name="weight_sums",
    )(*coset, up_own, up_other, att_own, att_other)


def spread_kernel(core_ref, own_ref, other_ref, out_ref):
    core = core_ref[0]
    rows, cols = own_ref.shape[0], out_ref.shape[2]
    mine = pl.ds(pl.multiple_of(core * cols, DH), cols)
    own, other = own_ref[:, mine], other_ref[:, mine]
    for n in range(out_ref.shape[0]):
        out_ref[n, pl.ds(pl.multiple_of(core * rows, rows), rows), :] = own
        out_ref[n, pl.ds(pl.multiple_of((1 - core) * rows, rows), rows), :] = other


def gather_weight(core, weight, other):
    rows, cols = weight.shape[0], weight.shape[1] // 2
    pieces = pl.pallas_call(
        spread_kernel,
        in_specs=[SMEM, VMEM, VMEM],
        out_specs=VMEM,
        out_shape=jax.ShapeDtypeStruct((16, 2 * rows, cols), BF),
        compiler_params=whole_params(LIMIT_SPREAD),
        name="spread",
    )(core, weight, other)
    block = lax.all_to_all(pieces, "d", 0, 0, axis_index_groups=CHIPS, tiled=True)
    return block.reshape(32 * rows, cols)


def split_kernel(block_ref, low_ref, high_ref):
    half = low_ref.shape[0]
    low_ref[...] = block_ref[:half, :]
    high_ref[...] = block_ref[half:, :]


def split(block):
    half = jax.ShapeDtypeStruct((block.shape[0] // 2, block.shape[1]), BF)
    return pl.pallas_call(
        split_kernel,
        in_specs=[VMEM],
        out_specs=[VMEM] * 2,
        out_shape=[half] * 2,
        compiler_params=whole_params(4),
        name="split",
    )(block)


def gather_cosets(block):
    parts = split(block)
    result = [block]
    for axis in range(3):
        for half in range(2):
            result.append(lax.ppermute(parts[half], "d", shift(axis, 2 * half - 1)))
    return result


def add_kernel(own_ref, *refs):
    received, out_ref = refs[:6], refs[6]
    rows = received[0].shape[0]
    for half in range(2):
        for lo in range(0, rows, 16):
            total = own_ref[rows * half + lo : rows * half + lo + 16, :].astype(F32)
            for axis in range(3):
                total = total + received[2 * axis + half][lo : lo + 16, :].astype(F32)
            out_ref[rows * half + lo : rows * half + lo + 16, :] = total.astype(BF)


def reduce_cosets(pieces):
    received = []
    for n, piece in enumerate(pieces[1:]):
        received.append(lax.ppermute(piece, "d", shift(n // 2, 1 - 2 * (n % 2))))
    return received


def add_received(own, received):
    return pl.pallas_call(
        add_kernel,
        in_specs=[VMEM] * 7,
        out_specs=VMEM,
        out_shape=jax.ShapeDtypeStruct(own.shape, BF),
        compiler_params=whole_params(LIMIT_SMALL),
        cost_estimate=pl.CostEstimate(flops=1 << 28, bytes_accessed=5 << 20, transcendentals=0),
        name="add_received",
    )(own, *received)


def own_rows_kernel(in_ref, out_ref, *, factor):
    cols = in_ref.shape[2]
    for half in range(2):
        total = in_ref[half].astype(F32)
        for n in range(1, in_ref.shape[0] // 2):
            total = total + in_ref[2 * n + half].astype(F32)
        out_ref[:, half * cols : (half + 1) * cols] = total * factor


def own_rows(rows_in, total_tokens):
    _, rows, cols = rows_in.shape
    return pl.pallas_call(
        functools.partial(own_rows_kernel, factor=1.0 / math.sqrt(total_tokens)),
        in_specs=[VMEM],
        out_specs=VMEM,
        out_shape=jax.ShapeDtypeStruct((rows, 2 * cols), F32),
        compiler_params=whole_params(LIMIT_SMALL),
        name="own_rows",
    )(rows_in)


def shards(queries, keys, values, upstream, weight, sample_ids):
    rows = queries.shape[0]
    me = lax.axis_index("d")
    core = jnp.bitwise_and(me, 1)
    z = jnp.bitwise_and(jnp.right_shift(me, 4), 1)
    kx = jnp.bitwise_and(jnp.right_shift(me, 5) + z, 1)
    ky = jnp.bitwise_and(jnp.right_shift(me, 1) + z, 1)
    coset = (kx.astype(jnp.int32).reshape(1), ky.astype(jnp.int32).reshape(1))
    steps = HALF // STEP_HEADS
    base_own = (steps * core).astype(jnp.int32).reshape(1)
    base_other = (steps * (1 - core)).astype(jnp.int32).reshape(1)

    up_other = lax.ppermute(upstream, "d", CORE_SWAP)
    other = lax.ppermute(weight, "d", CORE_SWAP)
    mine = gather_weight(core.astype(jnp.int32).reshape(1), weight, other)
    att_a, prob_a = attend_forward(
        base_other, queries, keys, values, sample_ids, LIMIT_A
    )
    att_other = lax.ppermute(att_a, "d", CORE_SWAP)
    att_b, prob_b = attend_forward(base_own, queries, keys, values, sample_ids, LIMIT)
    sums = weight_sums(coset, upstream, up_other, att_b, att_other)
    received = reduce_cosets(sums)
    mine, _ = lax.optimization_barrier((mine, sums[0]))
    gathered = gather_cosets(mine)
    reduced = add_received(sums[0], received)
    rows_in = exchange(reduced.reshape(32, -1, reduced.shape[1]))
    grad_own, grad_sent = project(coset, upstream, up_other, gathered)
    grad_other = lax.ppermute(grad_sent, "d", CORE_SWAP)
    outs = attend_backward(
        base_own, queries, keys, values, grad_own, att_b, prob_b, (), LIMIT_BACK
    )
    outs = attend_backward(
        base_other, queries, keys, values, grad_other, att_a, prob_a, tuple(outs), LIMIT_LAST
    )
    grad_weight = own_rows(rows_in, rows * lax.axis_size("d"))
    return (*outs, grad_weight)


def solution(mesh):
    flat = Mesh(mesh.devices.reshape(-1), ("d",))
    return jax.shard_map(
        shards,
        mesh=flat,
        in_specs=(P("d", None),) * 6,
        out_specs=(P("d", None),) * 4,
        check_vma=False,
    )
```

```python
import functools
import math

import jax
import jax.numpy as jnp
from jax import lax
from jax.experimental import pallas as pl
from jax.experimental.pallas import tpu as pltpu
from jax.sharding import Mesh
from jax.sharding import PartitionSpec as P


DH = 128
HALF = 8
STEP_HEADS = 4
LIMIT = 50
LIMIT_A = 60
LIMIT_BACK = 50
LIMIT_LAST = 50
LIMIT_PROJECT = 20
LIMIT_SUMS = 20
LIMIT_SMALL = 8
FLOPS_4US = 2 << 30
FLOPS_6US = 3 << 30
SCALE = 1.0 / math.sqrt(DH)
LOG2E = math.log2(math.e)
BF = jnp.bfloat16
F32 = jnp.float32
CLASSES = ((1, 0), (0, 1), (1, 1))


def coords(i):
    return (i // 32, (i // 2) % 4, 2 * ((i // 8) % 2) + (i // 16) % 2, i % 2)


def device_at(x, y, z, core):
    x, y, z = x % 4, y % 4, z % 4
    return x * 32 + (z % 2) * 16 + (z // 2) * 8 + y * 2 + core


COSETS = [
    [
        device_at((kx + z) % 2 + 2 * i, (ky + z) % 2 + 2 * j, z, core)
        for z in range(4)
        for i in range(2)
        for j in range(2)
        for core in range(2)
    ]
    for kx in range(2)
    for ky in range(2)
]
CORE_SWAP = [(i, i ^ 1) for i in range(128)]


def shift(axis, by):
    pairs = []
    for i in range(128):
        place = list(coords(i))
        place[axis] += by
        pairs.append((i, device_at(*place)))
    return pairs


def exchange(pieces):
    return lax.all_to_all(pieces, "d", 0, 0, axis_index_groups=COSETS, tiled=True)


def grid_params(mib):
    return pltpu.CompilerParams(
        dimension_semantics=("arbitrary",), vmem_limit_bytes=mib * 1024 * 1024
    )


def whole_params(mib):
    return pltpu.CompilerParams(vmem_limit_bytes=mib * 1024 * 1024)


BLOCK = 256
PACKED = 3 * BLOCK


def packed(i):
    return slice(0, BLOCK) if i == 0 else slice(BLOCK, PACKED)


def forward_kernel(base, q_ref, k_ref, v_ref, ids_ref, *refs):
    att_ref, prob_ref, bias_ref = refs[-3 - len(refs) // 4 : -1 - len(refs) // 4] + refs[-1:]
    rows = q_ref.shape[0]
    if len(refs) > 3:
        weight_ref, pieces_ref = refs[0], refs[3]
        cols = pieces_ref.shape[2]
        for n in range(pieces_ref.shape[0]):
            pieces_ref[n] = weight_ref[:, cols * (n % 2) : cols * (n % 2 + 1)]

    @pl.when(pl.program_id(0) == 0)
    def _():
        t = lax.broadcasted_iota(jnp.int32, (rows, rows), 0)
        u = lax.broadcasted_iota(jnp.int32, (rows, rows), 1)
        ids = ids_ref[...].astype(F32)
        own = jnp.broadcast_to(ids, (DH, rows)).T[:, :1]
        bias_ref[...] = jnp.where(jnp.logical_and(u <= t, own == ids), 0.0, -1e30)

    block = BLOCK

    def cut(h, i):
        return slice(h * DH, (h + 1) * DH), i * block, (i + 1) * block

    def scores_of(h, i):
        cols, lo, hi = cut(h, i)
        return lax.dot_general(
            q_ref[lo:hi, cols],
            k_ref[:hi, cols],
            (((1,), (1,)), ((), ())),
            preferred_element_type=F32,
        )

    def softmax_of(h, i, scores):
        _, lo, hi = cut(h, i)
        scores = scores * (SCALE * LOG2E) + bias_ref[lo:hi, :hi]
        raised = jnp.exp2(scores - jnp.max(scores, axis=1, keepdims=True))
        total = jnp.sum(raised, axis=1, keepdims=True)
        probs = (raised * (1.0 / total)).astype(BF)
        prob_ref[h, :, packed(i)] = probs
        return probs

    def attend(h, i, probs):
        cols, lo, hi = cut(h, i)
        att_ref[lo:hi, cols] = jnp.dot(
            probs, v_ref[:hi, cols], preferred_element_type=F32
        ).astype(BF)

    jobs = [(h, i) for h in range(STEP_HEADS) for i in range(rows // block)]
    ready = scores_of(*jobs[0])
    waiting = None
    for n, job in enumerate(jobs):
        scores = ready
        if n + 1 < len(jobs):
            ready = scores_of(*jobs[n + 1])
        probs = softmax_of(*job, scores)
        if waiting is not None:
            attend(*waiting)
        waiting = (*job, probs)
    attend(*waiting)


def attend_forward(base, queries, keys, values, ids, mib, weight=None):
    rows = queries.shape[0]
    steps = HALF // STEP_HEADS
    extra, extra_in, extra_out, extra_shape = (), [], [], []
    if weight is not None:
        wide = (32, weight.shape[0], weight.shape[1] // 2)
        extra = (weight,)
        extra_in = [pl.BlockSpec(weight.shape, lambda i, b: (0, 0))]
        extra_out = [pl.BlockSpec((wide[0] // steps, *wide[1:]), lambda i, b: (i, 0, 0))]
        extra_shape = [jax.ShapeDtypeStruct(wide, BF)]
    head = pl.BlockSpec((rows, DH * STEP_HEADS), lambda i, b: (0, b[0] + i))
    return pl.pallas_call(
        forward_kernel,
        grid_spec=pltpu.PrefetchScalarGridSpec(
            num_scalar_prefetch=1,
            grid=(steps,),
            in_specs=[head, head, head, pl.BlockSpec((1, rows), lambda i, b: (0, 0))] + extra_in,
            out_specs=[
                pl.BlockSpec((rows, DH * STEP_HEADS), lambda i, b: (0, i)),
                pl.BlockSpec((STEP_HEADS, BLOCK, PACKED), lambda i, b: (i, 0, 0)),
            ]
            + extra_out,
            scratch_shapes=[pltpu.VMEM((rows, rows), F32)],
        ),
        out_shape=[
            jax.ShapeDtypeStruct((rows, HALF * DH), BF),
            jax.ShapeDtypeStruct((HALF, BLOCK, PACKED), BF),
        ]
        + extra_shape,
        compiler_params=grid_params(mib),
        cost_estimate=pl.CostEstimate(
            flops=FLOPS_6US, bytes_accessed=9 << 20, transcendentals=1 << 20
        ),
        name="attend_forward",
    )(base, queries, keys, values, ids, *extra)


def backward_kernel(base, q_ref, k_ref, v_ref, g_ref, att_ref, prob_ref, *refs):
    dq_ref, dk_ref, dv_ref = refs[-3:]
    rows = q_ref.shape[0]
    block = BLOCK
    count = rows // block
    inner, grad_t, query_t, sums = {}, {}, {}, {}

    def cut(h, i):
        return slice(h * DH, (h + 1) * DH), i * block, (i + 1) * block

    def prepare(h):
        cols = cut(h, 0)[0]
        grad = g_ref[:, cols]
        inner[h] = jnp.sum(
            grad.astype(F32) * att_ref[:, cols].astype(F32), axis=1, keepdims=True
        )
        grad_t[h] = grad.T
        query_t[h] = q_ref[:, cols].T
        sums[h] = []

    def grad_probs_of(h, i):
        cols, lo, hi = cut(h, i)
        return lax.dot_general(
            g_ref[lo:hi, cols],
            v_ref[:hi, cols],
            (((1,), (1,)), ((), ())),
            preferred_element_type=F32,
        )

    def grad_scores_of(h, i, grad_probs):
        _, lo, hi = cut(h, i)
        probs = prob_ref[h, :, packed(i)].astype(F32)
        return (probs * (grad_probs - inner[h][lo:hi, :])).astype(BF)

    def finish(h, i, grad_scores):
        cols, lo, hi = cut(h, i)
        probs = prob_ref[h, :, packed(i)]
        dq_ref[lo:hi, cols] = (
            SCALE * jnp.dot(grad_scores, k_ref[:hi, cols], preferred_element_type=F32)
        ).astype(BF)
        sums[h].append(
            (
                jnp.dot(grad_t[h][:, lo:hi], probs, preferred_element_type=F32),
                jnp.dot(query_t[h][:, lo:hi], grad_scores, preferred_element_type=F32),
            )
        )
        if i < count - 1:
            return
        for n, (out_ref, factor) in enumerate(((dv_ref, 1.0), (dk_ref, SCALE))):
            for j in range(count):
                _, lo, hi = cut(h, j)
                total = sums[h][j][n][:, lo:hi]
                for m in range(j + 1, count):
                    total = total + sums[h][m][n][:, lo:hi]
                out_ref[lo:hi, cols] = (total * factor).astype(BF).T

    jobs = [(h, i) for h in range(STEP_HEADS) for i in range(count)]
    prepare(0)
    ready = grad_probs_of(*jobs[0])
    waiting = None
    for n, job in enumerate(jobs):
        grad_probs = ready
        if n + 1 < len(jobs):
            if jobs[n + 1][1] == 0:
                prepare(jobs[n + 1][0])
            ready = grad_probs_of(*jobs[n + 1])
        grad_scores = grad_scores_of(*job, grad_probs)
        if waiting is not None:
            finish(*waiting)
        waiting = (*job, grad_scores)
    finish(*waiting)


def attend_backward(base, queries, keys, values, grad, attended, probs, previous, mib):
    rows = queries.shape[0]
    head = pl.BlockSpec((rows, DH * STEP_HEADS), lambda i, b: (0, b[0] + i))
    half = pl.BlockSpec((rows, DH * STEP_HEADS), lambda i, b: (0, i))
    shape = jax.ShapeDtypeStruct(queries.shape, BF)
    return pl.pallas_call(
        backward_kernel,
        grid_spec=pltpu.PrefetchScalarGridSpec(
            num_scalar_prefetch=1,
            grid=(HALF // STEP_HEADS,),
            in_specs=[head, head, head, half, half]
            + [pl.BlockSpec((STEP_HEADS, BLOCK, PACKED), lambda i, b: (i, 0, 0))]
            + [pl.BlockSpec(memory_space=pl.ANY)] * len(previous),
            out_specs=[head, head, head],
        ),
        out_shape=[shape, shape, shape],
        input_output_aliases={7 + n: n for n in range(len(previous))},
        compiler_params=grid_params(mib),
        cost_estimate=pl.CostEstimate(
            flops=FLOPS_4US, bytes_accessed=12 << 20, transcendentals=0
        ),
        name="attend_backward",
    )(base, queries, keys, values, grad, attended, probs, *previous)


def row_of(coset, other, block):
    core, j, i, z = block % 2, (block // 2) % 2, (block // 4) % 2, block // 8
    odd_x, odd_y = (z + other[0]) % 2, (z + other[1]) % 2
    x = (1 - coset[0] if odd_x else coset[0]) + 2 * i
    y = (1 - coset[1] if odd_y else coset[1]) + 2 * j
    return 16 * (x * 32 + (z % 2) * 16 + (z // 2) * 8 + y * 2 + core)


def coset_parts():
    yield (0, 0), 0, 32
    for other in CLASSES:
        yield other, 0, 16
        yield other, 16, 32


def project_kernel(kx_ref, ky_ref, up_own_ref, up_other_ref, *refs):
    pieces, (own_ref, other_ref, weight_ref) = refs[:7], refs[7:]
    place = (kx_ref[0], ky_ref[0])
    for ref, (other, lo, hi) in zip(pieces, coset_parts()):
        for block in range(lo, hi):
            row = pl.multiple_of(row_of(place, other, block), 16)
            weight_ref[pl.ds(row, 16), :] = ref[16 * (block - lo) : 16 * (block - lo + 1), :]
    step = 512
    for up_ref, out_ref in ((up_other_ref, other_ref), (up_own_ref, own_ref)):
        for lo in range(0, out_ref.shape[1], step):
            out_ref[:, lo : lo + step] = jnp.dot(
                up_ref[...], weight_ref[:, lo : lo + step], preferred_element_type=F32
            ).astype(BF)


SMEM = pl.BlockSpec(memory_space=pltpu.SMEM)
HBM = pl.BlockSpec(memory_space=pltpu.HBM)
VMEM = pl.BlockSpec(memory_space=pltpu.VMEM)


def project(coset, up_own, up_other, pieces):
    rows, width = up_own.shape
    cols = pieces[0].shape[1]
    return pl.pallas_call(
        project_kernel,
        in_specs=[SMEM] * 2 + [VMEM] * (2 + len(pieces)),
        out_specs=[VMEM] * 2,
        out_shape=[jax.ShapeDtypeStruct((rows, cols), BF)] * 2,
        scratch_shapes=[pltpu.VMEM((width, cols), BF)],
        compiler_params=whole_params(LIMIT_PROJECT),
        cost_estimate=pl.CostEstimate(
            flops=FLOPS_4US, bytes_accessed=10 << 20, transcendentals=0
        ),
        name="project",
    )(*coset, up_own, up_other, *pieces)


def weight_kernel(kx_ref, ky_ref, up_own_ref, up_other_ref, att_own_ref, att_other_ref, *refs):
    own_ref, outs, stages, (sums_ref, out_sem) = refs[0], refs[1:7], refs[7:13], refs[13:]
    width = up_own_ref.shape[1]
    place = (kx_ref[0], ky_ref[0])
    step, cut = 256, 512

    def strip(lo):
        return jnp.concatenate(
            [up_own_ref[:, lo : lo + step].T, up_other_ref[:, lo : lo + step].T], axis=1
        )

    ready = strip(0)
    for lo in range(0, width, step):
        up_t = ready
        if lo + step < width:
            ready = strip(lo + step)
        for col in range(0, sums_ref.shape[1], cut):
            attended = jnp.concatenate(
                [att_own_ref[:, col : col + cut], att_other_ref[:, col : col + cut]], axis=0
            )
            sums_ref[lo : lo + step, col : col + cut] = jnp.dot(
                up_t, attended, preferred_element_type=F32
            ).astype(BF)
    copies = []
    for n, (other, lo, hi) in enumerate([*coset_parts()][1:] + [*coset_parts()][:1]):
        stage = stages[n] if n < len(stages) else own_ref
        for block in range(lo, hi):
            row = pl.multiple_of(row_of(place, other, block), 16)
            stage[16 * (block - lo) : 16 * (block - lo + 1), :] = sums_ref[pl.ds(row, 16), :]
        if n < len(stages):
            copies.append(pltpu.make_async_copy(stage, outs[n], out_sem.at[n]))
            copies[n].start()
    for copy in copies:
        copy.wait()


def weight_sums(coset, up_own, up_other, att_own, att_other):
    width = up_own.shape[1]
    cols = att_own.shape[1]
    sizes = [16 * (hi - lo) for _, lo, hi in coset_parts()]
    return pl.pallas_call(
        weight_kernel,
        in_specs=[SMEM] * 2 + [VMEM] * 4,
        out_specs=[VMEM] + [HBM] * (len(sizes) - 1),
        out_shape=[jax.ShapeDtypeStruct((size, cols), BF) for size in sizes],
        scratch_shapes=[pltpu.VMEM((size, cols), BF) for size in sizes[1:]]
        + [pltpu.VMEM((width, cols), BF), pltpu.SemaphoreType.DMA((len(sizes) - 1,))],
        compiler_params=whole_params(LIMIT_SUMS),
        cost_estimate=pl.CostEstimate(
            flops=FLOPS_4US, bytes_accessed=10 << 20, transcendentals=0
        ),
        name="weight_sums",
    )(*coset, up_own, up_other, att_own, att_other)


def split_kernel(block_ref, low_ref, high_ref):
    half = low_ref.shape[0]
    low_ref[...] = block_ref[:half, :]
    high_ref[...] = block_ref[half:, :]


def split(block):
    half = jax.ShapeDtypeStruct((block.shape[0] // 2, block.shape[1]), BF)
    return pl.pallas_call(
        split_kernel,
        in_specs=[VMEM],
        out_specs=[VMEM] * 2,
        out_shape=[half] * 2,
        compiler_params=whole_params(4),
        name="split",
    )(block)


def gather_cosets(block):
    parts = split(block)
    result = [block]
    for axis in range(3):
        for half in range(2):
            result.append(lax.ppermute(parts[half], "d", shift(axis, 2 * half - 1)))
    return result


def add_kernel(own_ref, *refs):
    received, out_ref = refs[:6], refs[6]
    rows = received[0].shape[0]
    for half in range(2):
        for lo in range(0, rows, 16):
            total = own_ref[rows * half + lo : rows * half + lo + 16, :].astype(F32)
            for axis in range(3):
                total = total + received[2 * axis + half][lo : lo + 16, :].astype(F32)
            out_ref[rows * half + lo : rows * half + lo + 16, :] = total.astype(BF)


def reduce_cosets(pieces):
    received = []
    for n, piece in enumerate(pieces[1:]):
        received.append(lax.ppermute(piece, "d", shift(n // 2, 1 - 2 * (n % 2))))
    return received


def add_received(own, received):
    return pl.pallas_call(
        add_kernel,
        in_specs=[VMEM] * 7,
        out_specs=VMEM,
        out_shape=jax.ShapeDtypeStruct(own.shape, BF),
        compiler_params=whole_params(LIMIT_SMALL),
        cost_estimate=pl.CostEstimate(flops=1 << 28, bytes_accessed=5 << 20, transcendentals=0),
        name="add_received",
    )(own, *received)


def own_rows_kernel(in_ref, out_ref, *, factor):
    cols = in_ref.shape[2]
    for half in range(2):
        total = in_ref[half].astype(F32)
        for n in range(1, in_ref.shape[0] // 2):
            total = total + in_ref[2 * n + half].astype(F32)
        out_ref[:, half * cols : (half + 1) * cols] = total * factor


def own_rows(rows_in, total_tokens):
    _, rows, cols = rows_in.shape
    return pl.pallas_call(
        functools.partial(own_rows_kernel, factor=1.0 / math.sqrt(total_tokens)),
        in_specs=[VMEM],
        out_specs=VMEM,
        out_shape=jax.ShapeDtypeStruct((rows, 2 * cols), F32),
        compiler_params=whole_params(LIMIT_SMALL),
        name="own_rows",
    )(rows_in)


def shards(queries, keys, values, upstream, weight, sample_ids):
    rows = queries.shape[0]
    me = lax.axis_index("d")
    core = jnp.bitwise_and(me, 1)
    z = jnp.bitwise_and(jnp.right_shift(me, 4), 1)
    kx = jnp.bitwise_and(jnp.right_shift(me, 5) + z, 1)
    ky = jnp.bitwise_and(jnp.right_shift(me, 1) + z, 1)
    coset = (kx.astype(jnp.int32).reshape(1), ky.astype(jnp.int32).reshape(1))
    steps = HALF // STEP_HEADS
    base_own = (steps * core).astype(jnp.int32).reshape(1)
    base_other = (steps * (1 - core)).astype(jnp.int32).reshape(1)

    up_other = lax.ppermute(upstream, "d", CORE_SWAP)
    att_a, prob_a, pieces = attend_forward(
        base_other, queries, keys, values, sample_ids, LIMIT_A, weight
    )
    mine = exchange(pieces).reshape(32 * weight.shape[0], -1)
    att_other = lax.ppermute(att_a, "d", CORE_SWAP)
    att_b, prob_b = attend_forward(base_own, queries, keys, values, sample_ids, LIMIT)
    sums = weight_sums(coset, upstream, up_other, att_b, att_other)
    received = reduce_cosets(sums)
    mine, _ = lax.optimization_barrier((mine, sums[0]))
    gathered = gather_cosets(mine)
    reduced = add_received(sums[0], received)
    rows_in = exchange(reduced.reshape(32, -1, reduced.shape[1]))
    grad_own, grad_sent = project(coset, upstream, up_other, gathered)
    grad_other = lax.ppermute(grad_sent, "d", CORE_SWAP)
    outs = attend_backward(base_own, queries, keys, values, grad_own, att_b, prob_b, (), LIMIT_BACK)
    outs = attend_backward(
        base_other, queries, keys, values, grad_other, att_a, prob_a, tuple(outs), LIMIT_LAST
    )
    grad_weight = own_rows(rows_in, rows * lax.axis_size("d"))
    return (*outs, grad_weight)


def solution(mesh):
    flat = Mesh(mesh.devices.reshape(-1), ("d",))
    return jax.shard_map(
        shards,
        mesh=flat,
        in_specs=(P("d", None),) * 6,
        out_specs=(P("d", None),) * 4,
        check_vma=False,
    )
```

```python
import functools
import math

import jax
import jax.numpy as jnp
from jax import lax
from jax.experimental import pallas as pl
from jax.experimental.pallas import tpu as pltpu
from jax.sharding import Mesh
from jax.sharding import PartitionSpec as P


DH = 128
HALF = 8
STEP_HEADS = 4
LIMIT = 50
LIMIT_A = 60
LIMIT_BACK = 60
LIMIT_LAST = 50
LIMIT_PROJECT = 50
LIMIT_ADD = 8
LIMIT_SUMS = 20
LIMIT_SMALL = 8
FLOPS_4US = 2 << 30
FLOPS_6US = 3 << 30
SCALE = 1.0 / math.sqrt(DH)
LOG2E = math.log2(math.e)
BF = jnp.bfloat16
F32 = jnp.float32
CLASSES = ((1, 0), (0, 1), (1, 1))


def coords(i):
    return (i // 32, (i // 2) % 4, 2 * ((i // 8) % 2) + (i // 16) % 2, i % 2)


def device_at(x, y, z, core):
    x, y, z = x % 4, y % 4, z % 4
    return x * 32 + (z % 2) * 16 + (z // 2) * 8 + y * 2 + core


COSETS = [
    [
        device_at((kx + z) % 2 + 2 * i, (ky + z) % 2 + 2 * j, z, core)
        for z in range(4)
        for i in range(2)
        for j in range(2)
        for core in range(2)
    ]
    for kx in range(2)
    for ky in range(2)
]
CORE_SWAP = [(i, i ^ 1) for i in range(128)]


def shift(axis, by):
    pairs = []
    for i in range(128):
        place = list(coords(i))
        place[axis] += by
        pairs.append((i, device_at(*place)))
    return pairs


def exchange(pieces):
    return lax.all_to_all(pieces, "d", 0, 0, axis_index_groups=COSETS, tiled=True)


def grid_params(mib):
    return pltpu.CompilerParams(
        dimension_semantics=("arbitrary",), vmem_limit_bytes=mib * 1024 * 1024
    )


def whole_params(mib):
    return pltpu.CompilerParams(vmem_limit_bytes=mib * 1024 * 1024)


BLOCK = 256
PACKED = 3 * BLOCK


def packed(i):
    return slice(0, BLOCK) if i == 0 else slice(BLOCK, PACKED)


def forward_kernel(base, q_ref, k_ref, v_ref, ids_ref, *refs):
    att_ref, prob_ref, bias_ref = refs[-3 - len(refs) // 4 : -1 - len(refs) // 4] + refs[-1:]
    rows = q_ref.shape[0]
    if len(refs) > 3:
        weight_ref, pieces_ref = refs[0], refs[3]
        cols = pieces_ref.shape[2]
        for n in range(pieces_ref.shape[0]):
            pieces_ref[n] = weight_ref[:, cols * (n % 2) : cols * (n % 2 + 1)]

    @pl.when(pl.program_id(0) == 0)
    def _():
        t = lax.broadcasted_iota(jnp.int32, (rows, rows), 0)
        u = lax.broadcasted_iota(jnp.int32, (rows, rows), 1)
        ids = ids_ref[...].astype(F32)
        own = jnp.broadcast_to(ids, (DH, rows)).T[:, :1]
        bias_ref[...] = jnp.where(jnp.logical_and(u <= t, own == ids), 0.0, -1e30)

    block = BLOCK

    def cut(h, i):
        return slice(h * DH, (h + 1) * DH), i * block, (i + 1) * block

    def scores_of(h, i):
        cols, lo, hi = cut(h, i)
        return lax.dot_general(
            q_ref[lo:hi, cols],
            k_ref[:hi, cols],
            (((1,), (1,)), ((), ())),
            preferred_element_type=F32,
        )

    def softmax_of(h, i, scores):
        _, lo, hi = cut(h, i)
        scores = scores * (SCALE * LOG2E) + bias_ref[lo:hi, :hi]
        raised = jnp.exp2(scores - jnp.max(scores, axis=1, keepdims=True))
        total = jnp.sum(raised, axis=1, keepdims=True)
        probs = (raised * (1.0 / total)).astype(BF)
        prob_ref[h, :, packed(i)] = probs
        return probs

    def attend(h, i, probs):
        cols, lo, hi = cut(h, i)
        att_ref[lo:hi, cols] = jnp.dot(
            probs, v_ref[:hi, cols], preferred_element_type=F32
        ).astype(BF)

    jobs = [(h, i) for h in range(STEP_HEADS) for i in range(rows // block)]
    ready = scores_of(*jobs[0])
    waiting = None
    for n, job in enumerate(jobs):
        scores = ready
        if n + 1 < len(jobs):
            ready = scores_of(*jobs[n + 1])
        probs = softmax_of(*job, scores)
        if waiting is not None:
            attend(*waiting)
        waiting = (*job, probs)
    attend(*waiting)


def attend_forward(base, queries, keys, values, ids, mib, weight=None):
    rows = queries.shape[0]
    steps = HALF // STEP_HEADS
    extra, extra_in, extra_out, extra_shape = (), [], [], []
    if weight is not None:
        wide = (32, weight.shape[0], weight.shape[1] // 2)
        extra = (weight,)
        extra_in = [pl.BlockSpec(weight.shape, lambda i, b: (0, 0))]
        extra_out = [pl.BlockSpec((wide[0] // steps, *wide[1:]), lambda i, b: (i, 0, 0))]
        extra_shape = [jax.ShapeDtypeStruct(wide, BF)]
    head = pl.BlockSpec((rows, DH * STEP_HEADS), lambda i, b: (0, b[0] + i))
    return pl.pallas_call(
        forward_kernel,
        grid_spec=pltpu.PrefetchScalarGridSpec(
            num_scalar_prefetch=1,
            grid=(steps,),
            in_specs=[head, head, head, pl.BlockSpec((1, rows), lambda i, b: (0, 0))] + extra_in,
            out_specs=[
                pl.BlockSpec((rows, DH * STEP_HEADS), lambda i, b: (0, i)),
                pl.BlockSpec((STEP_HEADS, BLOCK, PACKED), lambda i, b: (i, 0, 0)),
            ]
            + extra_out,
            scratch_shapes=[pltpu.VMEM((rows, rows), F32)],
        ),
        out_shape=[
            jax.ShapeDtypeStruct((rows, HALF * DH), BF),
            jax.ShapeDtypeStruct((HALF, BLOCK, PACKED), BF),
        ]
        + extra_shape,
        compiler_params=grid_params(mib),
        cost_estimate=pl.CostEstimate(
            flops=FLOPS_6US, bytes_accessed=9 << 20, transcendentals=1 << 20
        ),
        name="attend_forward",
    )(base, queries, keys, values, ids, *extra)


def backward_kernel(base, q_ref, k_ref, v_ref, g_ref, att_ref, prob_ref, *refs):
    dq_ref, dk_ref, dv_ref = refs[-3:]
    rows = q_ref.shape[0]
    block = BLOCK
    count = rows // block
    inner, grad_t, query_t, sums = {}, {}, {}, {}

    def cut(h, i):
        return slice(h * DH, (h + 1) * DH), i * block, (i + 1) * block

    def prepare(h):
        cols = cut(h, 0)[0]
        grad = g_ref[:, cols]
        inner[h] = jnp.sum(
            grad.astype(F32) * att_ref[:, cols].astype(F32), axis=1, keepdims=True
        )
        grad_t[h] = grad.T
        query_t[h] = q_ref[:, cols].T
        sums[h] = []

    def grad_probs_of(h, i):
        cols, lo, hi = cut(h, i)
        return lax.dot_general(
            g_ref[lo:hi, cols],
            v_ref[:hi, cols],
            (((1,), (1,)), ((), ())),
            preferred_element_type=F32,
        )

    def grad_scores_of(h, i, grad_probs):
        _, lo, hi = cut(h, i)
        probs = prob_ref[h, :, packed(i)].astype(F32)
        return (probs * (grad_probs - inner[h][lo:hi, :])).astype(BF)

    def finish(h, i, grad_scores):
        cols, lo, hi = cut(h, i)
        probs = prob_ref[h, :, packed(i)]
        dq_ref[lo:hi, cols] = (
            SCALE * jnp.dot(grad_scores, k_ref[:hi, cols], preferred_element_type=F32)
        ).astype(BF)
        sums[h].append(
            (
                jnp.dot(grad_t[h][:, lo:hi], probs, preferred_element_type=F32),
                jnp.dot(query_t[h][:, lo:hi], grad_scores, preferred_element_type=F32),
            )
        )
        if i < count - 1:
            return
        for n, (out_ref, factor) in enumerate(((dv_ref, 1.0), (dk_ref, SCALE))):
            for j in range(count):
                _, lo, hi = cut(h, j)
                total = sums[h][j][n][:, lo:hi]
                for m in range(j + 1, count):
                    total = total + sums[h][m][n][:, lo:hi]
                out_ref[lo:hi, cols] = (total * factor).astype(BF).T

    jobs = [(h, i) for h in range(STEP_HEADS) for i in range(count)]
    prepare(0)
    ready = grad_probs_of(*jobs[0])
    waiting = None
    for n, job in enumerate(jobs):
        grad_probs = ready
        if n + 1 < len(jobs):
            if jobs[n + 1][1] == 0:
                prepare(jobs[n + 1][0])
            ready = grad_probs_of(*jobs[n + 1])
        grad_scores = grad_scores_of(*job, grad_probs)
        if waiting is not None:
            finish(*waiting)
        waiting = (*job, grad_scores)
    finish(*waiting)


def attend_backward(base, queries, keys, values, grad, attended, probs, previous, mib):
    rows = queries.shape[0]
    head = pl.BlockSpec((rows, DH * STEP_HEADS), lambda i, b: (0, b[0] + i))
    half = pl.BlockSpec((rows, DH * STEP_HEADS), lambda i, b: (0, i))
    shape = jax.ShapeDtypeStruct(queries.shape, BF)
    return pl.pallas_call(
        backward_kernel,
        grid_spec=pltpu.PrefetchScalarGridSpec(
            num_scalar_prefetch=1,
            grid=(HALF // STEP_HEADS,),
            in_specs=[head, head, head, half, half]
            + [pl.BlockSpec((STEP_HEADS, BLOCK, PACKED), lambda i, b: (i, 0, 0))]
            + [pl.BlockSpec(memory_space=pl.ANY)] * len(previous),
            out_specs=[head, head, head],
        ),
        out_shape=[shape, shape, shape],
        input_output_aliases={7 + n: n for n in range(len(previous))},
        compiler_params=grid_params(mib),
        cost_estimate=pl.CostEstimate(
            flops=FLOPS_4US, bytes_accessed=12 << 20, transcendentals=0
        ),
        name="attend_backward",
    )(base, queries, keys, values, grad, attended, probs, *previous)


def row_of(coset, other, block):
    core, j, i, z = block % 2, (block // 2) % 2, (block // 4) % 2, block // 8
    odd_x, odd_y = (z + other[0]) % 2, (z + other[1]) % 2
    x = (1 - coset[0] if odd_x else coset[0]) + 2 * i
    y = (1 - coset[1] if odd_y else coset[1]) + 2 * j
    return 16 * (x * 32 + (z % 2) * 16 + (z // 2) * 8 + y * 2 + core)


def coset_parts():
    yield (0, 0), 0, 32
    for other in CLASSES:
        yield other, 0, 16
        yield other, 16, 32


def project_kernel(kx_ref, ky_ref, up_own_hbm, up_other_ref, *refs):
    pieces, (own_ref, other_ref, weight_ref, up_own_ref, sem) = refs[:7], refs[7:]
    load = pltpu.make_async_copy(up_own_hbm, up_own_ref, sem)
    load.start()
    place = (kx_ref[0], ky_ref[0])
    for ref, (other, lo, hi) in zip(pieces, coset_parts()):
        for block in range(lo, hi):
            row = pl.multiple_of(row_of(place, other, block), 16)
            weight_ref[pl.ds(row, 16), :] = ref[16 * (block - lo) : 16 * (block - lo + 1), :]
    step = 512
    for up_ref, out_ref in ((up_other_ref, other_ref), (up_own_ref, own_ref)):
        if up_ref is up_own_ref:
            load.wait()
        for lo in range(0, out_ref.shape[1], step):
            out_ref[:, lo : lo + step] = jnp.dot(
                up_ref[...], weight_ref[:, lo : lo + step], preferred_element_type=F32
            ).astype(BF)


SMEM = pl.BlockSpec(memory_space=pltpu.SMEM)
HBM = pl.BlockSpec(memory_space=pltpu.HBM)
VMEM = pl.BlockSpec(memory_space=pltpu.VMEM)


def project(coset, up_own, up_other, pieces):
    rows, width = up_own.shape
    cols = pieces[0].shape[1]
    return pl.pallas_call(
        project_kernel,
        in_specs=[SMEM, SMEM, HBM] + [VMEM] * (1 + len(pieces)),
        out_specs=[VMEM] * 2,
        out_shape=[jax.ShapeDtypeStruct((rows, cols), BF)] * 2,
        scratch_shapes=[
            pltpu.VMEM((width, cols), BF),
            pltpu.VMEM((rows, width), BF),
            pltpu.SemaphoreType.DMA,
        ],
        compiler_params=whole_params(LIMIT_PROJECT),
        cost_estimate=pl.CostEstimate(
            flops=FLOPS_4US, bytes_accessed=10 << 20, transcendentals=0
        ),
        name="project",
    )(*coset, up_own, up_other, *pieces)


def weight_kernel(kx_ref, ky_ref, up_own_ref, up_other_ref, att_own_ref, att_other_ref, *refs):
    own_ref, outs, stages, (sums_ref, out_sem) = refs[0], refs[1:7], refs[7:13], refs[13:]
    width = up_own_ref.shape[1]
    place = (kx_ref[0], ky_ref[0])
    step, cut = 256, 512

    def strip(lo):
        return jnp.concatenate(
            [up_own_ref[:, lo : lo + step].T, up_other_ref[:, lo : lo + step].T], axis=1
        )

    ready = strip(0)
    for lo in range(0, width, step):
        up_t = ready
        if lo + step < width:
            ready = strip(lo + step)
        for col in range(0, sums_ref.shape[1], cut):
            attended = jnp.concatenate(
                [att_own_ref[:, col : col + cut], att_other_ref[:, col : col + cut]], axis=0
            )
            sums_ref[lo : lo + step, col : col + cut] = jnp.dot(
                up_t, attended, preferred_element_type=F32
            ).astype(BF)
    copies = []
    for n, (other, lo, hi) in enumerate([*coset_parts()][1:] + [*coset_parts()][:1]):
        stage = stages[n] if n < len(stages) else own_ref
        for block in range(lo, hi):
            row = pl.multiple_of(row_of(place, other, block), 16)
            stage[16 * (block - lo) : 16 * (block - lo + 1), :] = sums_ref[pl.ds(row, 16), :]
        if n < len(stages):
            copies.append(pltpu.make_async_copy(stage, outs[n], out_sem.at[n]))
            copies[n].start()
    for copy in copies:
        copy.wait()


def weight_sums(coset, up_own, up_other, att_own, att_other):
    width = up_own.shape[1]
    cols = att_own.shape[1]
    sizes = [16 * (hi - lo) for _, lo, hi in coset_parts()]
    return pl.pallas_call(
        weight_kernel,
        in_specs=[SMEM] * 2 + [VMEM] * 4,
        out_specs=[VMEM] + [HBM] * (len(sizes) - 1),
        out_shape=[jax.ShapeDtypeStruct((size, cols), BF) for size in sizes],
        scratch_shapes=[pltpu.VMEM((size, cols), BF) for size in sizes[1:]]
        + [pltpu.VMEM((width, cols), BF), pltpu.SemaphoreType.DMA((len(sizes) - 1,))],
        compiler_params=whole_params(LIMIT_SUMS),
        cost_estimate=pl.CostEstimate(
            flops=FLOPS_4US, bytes_accessed=10 << 20, transcendentals=0
        ),
        name="weight_sums",
    )(*coset, up_own, up_other, att_own, att_other)


def split_kernel(block_ref, low_ref, high_ref):
    half = low_ref.shape[0]
    low_ref[...] = block_ref[:half, :]
    high_ref[...] = block_ref[half:, :]


def split(block):
    half = jax.ShapeDtypeStruct((block.shape[0] // 2, block.shape[1]), BF)
    return pl.pallas_call(
        split_kernel,
        in_specs=[VMEM],
        out_specs=[VMEM] * 2,
        out_shape=[half] * 2,
        compiler_params=whole_params(4),
        name="split",
    )(block)


def gather_cosets(block):
    parts = split(block)
    result = [block]
    for axis in range(3):
        for half in range(2):
            result.append(lax.ppermute(parts[half], "d", shift(axis, 2 * half - 1)))
    return result


ADD_STEPS = 4


def add_kernel(own_ref, *refs):
    received, out_ref = refs[:6], refs[6]

    def add(half):
        for lo in range(0, out_ref.shape[0], 16):
            rows = slice(lo, lo + 16)
            total = own_ref[rows, :].astype(F32)
            for axis in range(3):
                total = total + received[2 * axis + half][rows, :].astype(F32)
            out_ref[rows, :] = total.astype(BF)

    for half in range(2):
        pl.when(pl.program_id(0) // (ADD_STEPS // 2) == half)(functools.partial(add, half))


def reduce_cosets(pieces):
    received = []
    for n, piece in enumerate(pieces[1:]):
        received.append(lax.ppermute(piece, "d", shift(n // 2, 1 - 2 * (n % 2))))
    return received


def add_received(own, received):
    size = (own.shape[0] // ADD_STEPS, own.shape[1])
    last = ADD_STEPS // 2 - 1
    return pl.pallas_call(
        add_kernel,
        grid=(ADD_STEPS,),
        in_specs=[pl.BlockSpec(size, lambda i: (i, 0))]
        + [
            pl.BlockSpec(size, lambda i: (jnp.minimum(i, last), 0)),
            pl.BlockSpec(size, lambda i: (jnp.maximum(i - last - 1, 0), 0)),
        ]
        * 3,
        out_specs=pl.BlockSpec(size, lambda i: (i, 0)),
        out_shape=jax.ShapeDtypeStruct(own.shape, BF),
        compiler_params=grid_params(LIMIT_ADD),
        cost_estimate=pl.CostEstimate(flops=1 << 28, bytes_accessed=5 << 20, transcendentals=0),
        name="add_received",
    )(own, *received)


def own_rows_kernel(in_ref, out_ref, *, factor):
    cols = in_ref.shape[2]
    for half in range(2):
        total = in_ref[half].astype(F32)
        for n in range(1, in_ref.shape[0] // 2):
            total = total + in_ref[2 * n + half].astype(F32)
        out_ref[:, half * cols : (half + 1) * cols] = total * factor


def own_rows(rows_in, total_tokens):
    _, rows, cols = rows_in.shape
    return pl.pallas_call(
        functools.partial(own_rows_kernel, factor=1.0 / math.sqrt(total_tokens)),
        in_specs=[VMEM],
        out_specs=VMEM,
        out_shape=jax.ShapeDtypeStruct((rows, 2 * cols), F32),
        compiler_params=whole_params(LIMIT_SMALL),
        name="own_rows",
    )(rows_in)


def shards(queries, keys, values, upstream, weight, sample_ids):
    rows = queries.shape[0]
    me = lax.axis_index("d")
    core = jnp.bitwise_and(me, 1)
    z = jnp.bitwise_and(jnp.right_shift(me, 4), 1)
    kx = jnp.bitwise_and(jnp.right_shift(me, 5) + z, 1)
    ky = jnp.bitwise_and(jnp.right_shift(me, 1) + z, 1)
    coset = (kx.astype(jnp.int32).reshape(1), ky.astype(jnp.int32).reshape(1))
    steps = HALF // STEP_HEADS
    base_own = (steps * core).astype(jnp.int32).reshape(1)
    base_other = (steps * (1 - core)).astype(jnp.int32).reshape(1)

    up_other = lax.ppermute(upstream, "d", CORE_SWAP)
    att_a, prob_a, pieces = attend_forward(
        base_other, queries, keys, values, sample_ids, LIMIT_A, weight
    )
    mine = exchange(pieces).reshape(32 * weight.shape[0], -1)
    att_other = lax.ppermute(att_a, "d", CORE_SWAP)
    att_b, prob_b = attend_forward(base_own, queries, keys, values, sample_ids, LIMIT)
    sums = weight_sums(coset, upstream, up_other, att_b, att_other)
    received = reduce_cosets(sums)
    mine, _ = lax.optimization_barrier((mine, sums[0]))
    gathered = gather_cosets(mine)
    reduced = add_received(sums[0], received)
    rows_in = exchange(reduced.reshape(32, -1, reduced.shape[1]))
    grad_own, grad_sent = project(coset, upstream, up_other, gathered)
    grad_other = lax.ppermute(grad_sent, "d", CORE_SWAP)
    outs = attend_backward(base_own, queries, keys, values, grad_own, att_b, prob_b, (), LIMIT_BACK)
    outs = attend_backward(
        base_other, queries, keys, values, grad_other, att_a, prob_a, tuple(outs), LIMIT_LAST
    )
    grad_weight = own_rows(rows_in, rows * lax.axis_size("d"))
    return (*outs, grad_weight)


def solution(mesh):
    flat = Mesh(mesh.devices.reshape(-1), ("d",))
    return jax.shard_map(
        shards,
        mesh=flat,
        in_specs=(P("d", None),) * 6,
        out_specs=(P("d", None),) * 4,
        check_vma=False,
    )
```

```python
import functools
import math

import jax
import jax.numpy as jnp
from jax import lax
from jax.experimental import pallas as pl
from jax.experimental.pallas import tpu as pltpu
from jax.sharding import Mesh
from jax.sharding import PartitionSpec as P


DH = 128
HALF = 8
STEP_HEADS = 4
LIMIT = 50
LIMIT_A = 60
LIMIT_BACK = 60
LIMIT_LAST = 50
LIMIT_PROJECT = 54
LIMIT_SUMS = 20
LIMIT_SMALL = 8
FLOPS_4US = 2 << 30
FLOPS_6US = 3 << 30
SCALE = 1.0 / math.sqrt(DH)
LOG2E = math.log2(math.e)
BF = jnp.bfloat16
F32 = jnp.float32
CLASSES = ((1, 0), (0, 1), (1, 1))


def coords(i):
    return (i // 32, (i // 2) % 4, 2 * ((i // 8) % 2) + (i // 16) % 2, i % 2)


def device_at(x, y, z, core):
    x, y, z = x % 4, y % 4, z % 4
    return x * 32 + (z % 2) * 16 + (z // 2) * 8 + y * 2 + core


COSETS = [
    [
        device_at((kx + z) % 2 + 2 * i, (ky + z) % 2 + 2 * j, z, core)
        for z in range(4)
        for i in range(2)
        for j in range(2)
        for core in range(2)
    ]
    for kx in range(2)
    for ky in range(2)
]
CORE_SWAP = [(i, i ^ 1) for i in range(128)]


def shift(axis, by):
    pairs = []
    for i in range(128):
        place = list(coords(i))
        place[axis] += by
        pairs.append((i, device_at(*place)))
    return pairs


def exchange(pieces):
    return lax.all_to_all(pieces, "d", 0, 0, axis_index_groups=COSETS, tiled=True)


def grid_params(mib):
    return pltpu.CompilerParams(
        dimension_semantics=("arbitrary",), vmem_limit_bytes=mib * 1024 * 1024
    )


def whole_params(mib):
    return pltpu.CompilerParams(vmem_limit_bytes=mib * 1024 * 1024)


BLOCK = 256
PACKED = 3 * BLOCK


def packed(i):
    return slice(0, BLOCK) if i == 0 else slice(BLOCK, PACKED)


def forward_kernel(base, q_ref, k_ref, v_ref, ids_ref, *refs):
    att_ref, prob_ref, bias_ref = refs[-3 - len(refs) // 4 : -1 - len(refs) // 4] + refs[-1:]
    rows = q_ref.shape[0]
    if len(refs) > 3:
        weight_ref, pieces_ref = refs[0], refs[3]
        cols = pieces_ref.shape[2]
        for n in range(pieces_ref.shape[0]):
            pieces_ref[n] = weight_ref[:, cols * (n % 2) : cols * (n % 2 + 1)]

    @pl.when(pl.program_id(0) == 0)
    def _():
        t = lax.broadcasted_iota(jnp.int32, (rows, rows), 0)
        u = lax.broadcasted_iota(jnp.int32, (rows, rows), 1)
        ids = ids_ref[...].astype(F32)
        own = jnp.broadcast_to(ids, (DH, rows)).T[:, :1]
        bias_ref[...] = jnp.where(jnp.logical_and(u <= t, own == ids), 0.0, -1e30)

    block = BLOCK

    def cut(h, i):
        return slice(h * DH, (h + 1) * DH), i * block, (i + 1) * block

    def scores_of(h, i):
        cols, lo, hi = cut(h, i)
        return lax.dot_general(
            q_ref[lo:hi, cols],
            k_ref[:hi, cols],
            (((1,), (1,)), ((), ())),
            preferred_element_type=F32,
        )

    def softmax_of(h, i, scores):
        _, lo, hi = cut(h, i)
        scores = scores * (SCALE * LOG2E) + bias_ref[lo:hi, :hi]
        raised = jnp.exp2(scores - jnp.max(scores, axis=1, keepdims=True))
        total = jnp.sum(raised, axis=1, keepdims=True)
        probs = (raised * (1.0 / total)).astype(BF)
        prob_ref[h, :, packed(i)] = probs
        return probs

    def attend(h, i, probs):
        cols, lo, hi = cut(h, i)
        att_ref[lo:hi, cols] = jnp.dot(
            probs, v_ref[:hi, cols], preferred_element_type=F32
        ).astype(BF)

    jobs = [(h, i) for h in range(STEP_HEADS) for i in range(rows // block)]
    ready = scores_of(*jobs[0])
    waiting = None
    for n, job in enumerate(jobs):
        scores = ready
        if n + 1 < len(jobs):
            ready = scores_of(*jobs[n + 1])
        probs = softmax_of(*job, scores)
        if waiting is not None:
            attend(*waiting)
        waiting = (*job, probs)
    attend(*waiting)


def attend_forward(base, queries, keys, values, ids, mib, weight=None):
    rows = queries.shape[0]
    steps = HALF // STEP_HEADS
    extra, extra_in, extra_out, extra_shape = (), [], [], []
    if weight is not None:
        wide = (32, weight.shape[0], weight.shape[1] // 2)
        extra = (weight,)
        extra_in = [pl.BlockSpec(weight.shape, lambda i, b: (0, 0))]
        extra_out = [pl.BlockSpec((wide[0] // steps, *wide[1:]), lambda i, b: (i, 0, 0))]
        extra_shape = [jax.ShapeDtypeStruct(wide, BF)]
    head = pl.BlockSpec((rows, DH * STEP_HEADS), lambda i, b: (0, b[0] + i))
    return pl.pallas_call(
        forward_kernel,
        grid_spec=pltpu.PrefetchScalarGridSpec(
            num_scalar_prefetch=1,
            grid=(steps,),
            in_specs=[head, head, head, pl.BlockSpec((1, rows), lambda i, b: (0, 0))] + extra_in,
            out_specs=[
                pl.BlockSpec((rows, DH * STEP_HEADS), lambda i, b: (0, i)),
                pl.BlockSpec((STEP_HEADS, BLOCK, PACKED), lambda i, b: (i, 0, 0)),
            ]
            + extra_out,
            scratch_shapes=[pltpu.VMEM((rows, rows), F32)],
        ),
        out_shape=[
            jax.ShapeDtypeStruct((rows, HALF * DH), BF),
            jax.ShapeDtypeStruct((HALF, BLOCK, PACKED), BF),
        ]
        + extra_shape,
        compiler_params=grid_params(mib),
        cost_estimate=pl.CostEstimate(
            flops=FLOPS_6US, bytes_accessed=9 << 20, transcendentals=1 << 20
        ),
        name="attend_forward",
    )(base, queries, keys, values, ids, *extra)


def backward_kernel(base, q_ref, k_ref, v_ref, g_ref, att_ref, prob_ref, *refs):
    dq_ref, dk_ref, dv_ref = refs[-3:]
    rows = q_ref.shape[0]
    block = BLOCK
    count = rows // block
    inner, grad_t, query_t, sums = {}, {}, {}, {}

    def cut(h, i):
        return slice(h * DH, (h + 1) * DH), i * block, (i + 1) * block

    def prepare(h):
        cols = cut(h, 0)[0]
        grad = g_ref[:, cols]
        inner[h] = jnp.sum(
            grad.astype(F32) * att_ref[:, cols].astype(F32), axis=1, keepdims=True
        )
        grad_t[h] = grad.T
        query_t[h] = q_ref[:, cols].T
        sums[h] = []

    def grad_probs_of(h, i):
        cols, lo, hi = cut(h, i)
        return lax.dot_general(
            g_ref[lo:hi, cols],
            v_ref[:hi, cols],
            (((1,), (1,)), ((), ())),
            preferred_element_type=F32,
        )

    def grad_scores_of(h, i, grad_probs):
        _, lo, hi = cut(h, i)
        probs = prob_ref[h, :, packed(i)].astype(F32)
        return (probs * (grad_probs - inner[h][lo:hi, :])).astype(BF)

    def finish(h, i, grad_scores):
        cols, lo, hi = cut(h, i)
        probs = prob_ref[h, :, packed(i)]
        dq_ref[lo:hi, cols] = (
            SCALE * jnp.dot(grad_scores, k_ref[:hi, cols], preferred_element_type=F32)
        ).astype(BF)
        sums[h].append(
            (
                jnp.dot(grad_t[h][:, lo:hi], probs, preferred_element_type=F32),
                jnp.dot(query_t[h][:, lo:hi], grad_scores, preferred_element_type=F32),
            )
        )
        if i < count - 1:
            return
        for n, (out_ref, factor) in enumerate(((dv_ref, 1.0), (dk_ref, SCALE))):
            for j in range(count):
                _, lo, hi = cut(h, j)
                total = sums[h][j][n][:, lo:hi]
                for m in range(j + 1, count):
                    total = total + sums[h][m][n][:, lo:hi]
                out_ref[lo:hi, cols] = (total * factor).astype(BF).T

    jobs = [(h, i) for h in range(STEP_HEADS) for i in range(count)]
    prepare(0)
    ready = grad_probs_of(*jobs[0])
    waiting = None
    for n, job in enumerate(jobs):
        grad_probs = ready
        if n + 1 < len(jobs):
            if jobs[n + 1][1] == 0:
                prepare(jobs[n + 1][0])
            ready = grad_probs_of(*jobs[n + 1])
        grad_scores = grad_scores_of(*job, grad_probs)
        if waiting is not None:
            finish(*waiting)
        waiting = (*job, grad_scores)
    finish(*waiting)


def attend_backward(base, queries, keys, values, grad, attended, probs, previous, mib):
    rows = queries.shape[0]
    head = pl.BlockSpec((rows, DH * STEP_HEADS), lambda i, b: (0, b[0] + i))
    half = pl.BlockSpec((rows, DH * STEP_HEADS), lambda i, b: (0, i))
    shape = jax.ShapeDtypeStruct(queries.shape, BF)
    return pl.pallas_call(
        backward_kernel,
        grid_spec=pltpu.PrefetchScalarGridSpec(
            num_scalar_prefetch=1,
            grid=(HALF // STEP_HEADS,),
            in_specs=[head, head, head, half, half]
            + [pl.BlockSpec((STEP_HEADS, BLOCK, PACKED), lambda i, b: (i, 0, 0))]
            + [pl.BlockSpec(memory_space=pl.ANY)] * len(previous),
            out_specs=[head, head, head],
        ),
        out_shape=[shape, shape, shape],
        input_output_aliases={7 + n: n for n in range(len(previous))},
        compiler_params=grid_params(mib),
        cost_estimate=pl.CostEstimate(
            flops=FLOPS_4US, bytes_accessed=12 << 20, transcendentals=0
        ),
        name="attend_backward",
    )(base, queries, keys, values, grad, attended, probs, *previous)


def row_of(coset, other, block):
    core, j, i, z = block % 2, (block // 2) % 2, (block // 4) % 2, block // 8
    odd_x, odd_y = (z + other[0]) % 2, (z + other[1]) % 2
    x = (1 - coset[0] if odd_x else coset[0]) + 2 * i
    y = (1 - coset[1] if odd_y else coset[1]) + 2 * j
    return 16 * (x * 32 + (z % 2) * 16 + (z // 2) * 8 + y * 2 + core)


def coset_parts():
    yield (0, 0), 0, 32
    for other in CLASSES:
        yield other, 0, 16
        yield other, 16, 32


def project_kernel(kx_ref, ky_ref, up_own_hbm, up_other_ref, *refs):
    pieces, (own_ref, other_ref, weight_ref, up_own_ref, sem) = refs[:7], refs[7:]
    load = pltpu.make_async_copy(up_own_hbm, up_own_ref, sem)
    load.start()
    place = (kx_ref[0], ky_ref[0])
    for ref, (other, lo, hi) in zip(pieces, coset_parts()):
        for block in range(lo, hi):
            row = pl.multiple_of(row_of(place, other, block), 16)
            weight_ref[pl.ds(row, 16), :] = ref[16 * (block - lo) : 16 * (block - lo + 1), :]
    step = 512
    for up_ref, out_ref in ((up_other_ref, other_ref), (up_own_ref, own_ref)):
        if up_ref is up_own_ref:
            load.wait()
        for lo in range(0, out_ref.shape[1], step):
            out_ref[:, lo : lo + step] = jnp.dot(
                up_ref[...], weight_ref[:, lo : lo + step], preferred_element_type=F32
            ).astype(BF)


SMEM = pl.BlockSpec(memory_space=pltpu.SMEM)
HBM = pl.BlockSpec(memory_space=pltpu.HBM)
VMEM = pl.BlockSpec(memory_space=pltpu.VMEM)


def project(coset, up_own, up_other, pieces):
    rows, width = up_own.shape
    cols = pieces[0].shape[1]
    return pl.pallas_call(
        project_kernel,
        in_specs=[SMEM, SMEM, HBM] + [VMEM] * (1 + len(pieces)),
        out_specs=[VMEM] * 2,
        out_shape=[jax.ShapeDtypeStruct((rows, cols), BF)] * 2,
        scratch_shapes=[
            pltpu.VMEM((width, cols), BF),
            pltpu.VMEM((rows, width), BF),
            pltpu.SemaphoreType.DMA,
        ],
        compiler_params=whole_params(LIMIT_PROJECT),
        cost_estimate=pl.CostEstimate(
            flops=FLOPS_4US, bytes_accessed=10 << 20, transcendentals=0
        ),
        name="project",
    )(*coset, up_own, up_other, *pieces)


def weight_kernel(kx_ref, ky_ref, up_own_ref, up_other_ref, att_own_ref, att_other_ref, *refs):
    own_ref, outs, stages, (sums_ref, out_sem) = refs[0], refs[1:7], refs[7:13], refs[13:]
    width = up_own_ref.shape[1]
    place = (kx_ref[0], ky_ref[0])
    step, cut = 256, 512

    def strip(lo):
        return jnp.concatenate(
            [up_own_ref[:, lo : lo + step].T, up_other_ref[:, lo : lo + step].T], axis=1
        )

    ready = strip(0)
    for lo in range(0, width, step):
        up_t = ready
        if lo + step < width:
            ready = strip(lo + step)
        for col in range(0, sums_ref.shape[1], cut):
            attended = jnp.concatenate(
                [att_own_ref[:, col : col + cut], att_other_ref[:, col : col + cut]], axis=0
            )
            sums_ref[lo : lo + step, col : col + cut] = jnp.dot(
                up_t, attended, preferred_element_type=F32
            ).astype(BF)
    copies = []
    for n, (other, lo, hi) in enumerate([*coset_parts()][1:] + [*coset_parts()][:1]):
        stage = stages[n] if n < len(stages) else own_ref
        for block in range(lo, hi):
            row = pl.multiple_of(row_of(place, other, block), 16)
            stage[16 * (block - lo) : 16 * (block - lo + 1), :] = sums_ref[pl.ds(row, 16), :]
        if n < len(stages):
            copies.append(pltpu.make_async_copy(stage, outs[n], out_sem.at[n]))
            copies[n].start()
    for copy in copies:
        copy.wait()


def weight_sums(coset, up_own, up_other, att_own, att_other):
    width = up_own.shape[1]
    cols = att_own.shape[1]
    sizes = [16 * (hi - lo) for _, lo, hi in coset_parts()]
    return pl.pallas_call(
        weight_kernel,
        in_specs=[SMEM] * 2 + [VMEM] * 4,
        out_specs=[VMEM] + [HBM] * (len(sizes) - 1),
        out_shape=[jax.ShapeDtypeStruct((size, cols), BF) for size in sizes],
        scratch_shapes=[pltpu.VMEM((size, cols), BF) for size in sizes[1:]]
        + [pltpu.VMEM((width, cols), BF), pltpu.SemaphoreType.DMA((len(sizes) - 1,))],
        compiler_params=whole_params(LIMIT_SUMS),
        cost_estimate=pl.CostEstimate(
            flops=FLOPS_4US, bytes_accessed=10 << 20, transcendentals=0
        ),
        name="weight_sums",
    )(*coset, up_own, up_other, att_own, att_other)


def split_kernel(block_ref, low_ref, high_ref):
    half = low_ref.shape[0]
    low_ref[...] = block_ref[:half, :]
    high_ref[...] = block_ref[half:, :]


def split(block):
    half = jax.ShapeDtypeStruct((block.shape[0] // 2, block.shape[1]), BF)
    return pl.pallas_call(
        split_kernel,
        in_specs=[VMEM],
        out_specs=[VMEM] * 2,
        out_shape=[half] * 2,
        compiler_params=whole_params(4),
        name="split",
    )(block)


def gather_cosets(block):
    parts = split(block)
    result = [block]
    for axis in range(3):
        for half in range(2):
            result.append(lax.ppermute(parts[half], "d", shift(axis, 2 * half - 1)))
    return result


def add_kernel(own_ref, *refs):
    received, out_ref = refs[:6], refs[6]
    rows = received[0].shape[0]
    for half in range(2):
        for lo in range(0, rows, 16):
            total = own_ref[rows * half + lo : rows * half + lo + 16, :].astype(F32)
            for axis in range(3):
                total = total + received[2 * axis + half][lo : lo + 16, :].astype(F32)
            out_ref[rows * half + lo : rows * half + lo + 16, :] = total.astype(BF)


def reduce_cosets(pieces):
    received = []
    for n, piece in enumerate(pieces[1:]):
        received.append(lax.ppermute(piece, "d", shift(n // 2, 1 - 2 * (n % 2))))
    return received


def add_received(own, received):
    return pl.pallas_call(
        add_kernel,
        in_specs=[VMEM] * 7,
        out_specs=VMEM,
        out_shape=jax.ShapeDtypeStruct(own.shape, BF),
        compiler_params=whole_params(LIMIT_SMALL),
        cost_estimate=pl.CostEstimate(flops=1 << 28, bytes_accessed=5 << 20, transcendentals=0),
        name="add_received",
    )(own, *received)


def own_rows_kernel(in_ref, out_ref, *, factor):
    cols = in_ref.shape[2]
    for half in range(2):
        total = in_ref[half].astype(F32)
        for n in range(1, in_ref.shape[0] // 2):
            total = total + in_ref[2 * n + half].astype(F32)
        out_ref[:, half * cols : (half + 1) * cols] = total * factor


def own_rows(rows_in, total_tokens):
    _, rows, cols = rows_in.shape
    return pl.pallas_call(
        functools.partial(own_rows_kernel, factor=1.0 / math.sqrt(total_tokens)),
        in_specs=[VMEM],
        out_specs=VMEM,
        out_shape=jax.ShapeDtypeStruct((rows, 2 * cols), F32),
        compiler_params=whole_params(LIMIT_SMALL),
        name="own_rows",
    )(rows_in)


def shards(queries, keys, values, upstream, weight, sample_ids):
    rows = queries.shape[0]
    me = lax.axis_index("d")
    core = jnp.bitwise_and(me, 1)
    z = jnp.bitwise_and(jnp.right_shift(me, 4), 1)
    kx = jnp.bitwise_and(jnp.right_shift(me, 5) + z, 1)
    ky = jnp.bitwise_and(jnp.right_shift(me, 1) + z, 1)
    coset = (kx.astype(jnp.int32).reshape(1), ky.astype(jnp.int32).reshape(1))
    steps = HALF // STEP_HEADS
    base_own = (steps * core).astype(jnp.int32).reshape(1)
    base_other = (steps * (1 - core)).astype(jnp.int32).reshape(1)

    up_other = lax.ppermute(upstream, "d", CORE_SWAP)
    att_a, prob_a, pieces = attend_forward(
        base_other, queries, keys, values, sample_ids, LIMIT_A, weight
    )
    mine = exchange(pieces).reshape(32 * weight.shape[0], -1)
    att_other = lax.ppermute(att_a, "d", CORE_SWAP)
    att_b, prob_b = attend_forward(base_own, queries, keys, values, sample_ids, LIMIT)
    sums = weight_sums(coset, upstream, up_other, att_b, att_other)
    received = reduce_cosets(sums)
    mine, _ = lax.optimization_barrier((mine, sums[0]))
    gathered = gather_cosets(mine)
    reduced = add_received(sums[0], received)
    rows_in = exchange(reduced.reshape(32, -1, reduced.shape[1]))
    grad_own, grad_sent = project(coset, upstream, up_other, gathered)
    grad_other = lax.ppermute(grad_sent, "d", CORE_SWAP)
    outs = attend_backward(base_own, queries, keys, values, grad_own, att_b, prob_b, (), LIMIT_BACK)
    outs = attend_backward(
        base_other, queries, keys, values, grad_other, att_a, prob_a, tuple(outs), LIMIT_LAST
    )
    grad_weight = own_rows(rows_in, rows * lax.axis_size("d"))
    return (*outs, grad_weight)


def solution(mesh):
    flat = Mesh(mesh.devices.reshape(-1), ("d",))
    return jax.shard_map(
        shards,
        mesh=flat,
        in_specs=(P("d", None),) * 6,
        out_specs=(P("d", None),) * 4,
        check_vma=False,
    )
```
